32 devices in a mesh: tp: 1 (over z), cp: 32 (over y, x, core).
Axes of the slice: x: 4, y: 4, z: 1, core: 2. Of those that a mesh axis runs over, the one named last changes fastest.
The devices are a block of a 4x4x8 slice.
Arguments:
- query: bfloat16 [32, 256, 4, 128], P(None, 'cp', 'tp')
- out_act: bfloat16 [32, 256, 4, 128], P(None, 'cp', 'tp')
- out_grad: bfloat16 [32, 256, 4, 128], P(None, 'cp', 'tp')
- row_lse: float32 [32, 256, 4], P(None, 'cp', 'tp')
- key_act: bfloat16 [24576, 1, 128], P('cp', 'tp')
- value_act: bfloat16 [24576, 1, 128], P('cp', 'tp')
- doc_ids: int32 [24576], replicated
Outputs:
- output 1: bfloat16 [32, 256, 4, 128], P(None, 'cp', 'tp')
- output 2: float32 [24576, 1, 128], P('cp', 'tp')
- output 3: float32 [24576, 1, 128], P('cp', 'tp')
All inputs are finite; a program needn't handle non-finite values.
Results may differ from the reference program's by a relative error of at most 0.001.
Values are sent between devices in bfloat16 or wider.
A program may use at most 768 MiB of HBM per device.

```python
import jax
import jax.numpy as jnp
from jax import lax

SLICES = 32
SUB_LEN = 256
PRE_LEN = 16384
Q_HEADS = 4
KV_HEADS = 1
HEAD_DIM = 128
SPLITS = 32

PREFIX = PRE_LEN + SLICES * SUB_LEN
GROUP_SIZE = Q_HEADS // KV_HEADS
BLOCK_LEN = SUB_LEN // SPLITS
SCORE_SCALE = HEAD_DIM ** -0.5
GRAD_SCALE = (PREFIX // 8) ** 0.5
DOC_MEAN = PREFIX // 8


def masked_scores(q_blk, key_act, doc_ids, first_pos):
    block_len = q_blk.shape[0]
    scores = jnp.einsum('qhgd,khd->qhgk', q_blk.astype(jnp.float32), key_act.astype(jnp.float32)) * SCORE_SCALE
    q_pos = first_pos + jnp.arange(block_len)
    k_pos = jnp.arange(key_act.shape[0])
    q_doc = lax.dynamic_slice(doc_ids, (first_pos,), (block_len,))
    allowed = (k_pos[None, :] <= q_pos[:, None]) & (doc_ids[None, :] == q_doc[:, None])
    return scores, allowed[:, None, None, :]


def forward_lse(query, key_act, doc_ids):
    n_blocks = SLICES * SPLITS
    q_blocks = query.reshape(n_blocks, BLOCK_LEN, KV_HEADS, GROUP_SIZE, HEAD_DIM)
    firsts = PRE_LEN + jnp.arange(n_blocks) * BLOCK_LEN

    def block_lse(xs_blk):
        q_blk, first_pos = xs_blk
        scores, allowed = masked_scores(q_blk, key_act, doc_ids, first_pos)
        return jax.nn.logsumexp(jnp.where(allowed, scores, -1e30), axis=-1)

    return lax.map(block_lse, (q_blocks, firsts)).reshape(SLICES, SUB_LEN, Q_HEADS)


def setup_inputs(seed: int = 0, part: int = 0) -> dict:
    root_key = jax.random.key(seed)
    part_keys = jax.random.split(jax.random.fold_in(root_key, part), 5)
    doc_key = jax.random.key(seed + 17)
    starts = (jax.random.randint(doc_key, (PREFIX,), 0, DOC_MEAN) == 0) & (jnp.arange(PREFIX) > 0)
    doc_ids = jnp.cumsum(starts.astype(jnp.int32)).astype(jnp.int32)
    q_shape = (SLICES, SUB_LEN, Q_HEADS, HEAD_DIM)
    query = jax.random.normal(part_keys[0], q_shape, jnp.float32).astype(jnp.bfloat16)
    key_act = jax.random.normal(part_keys[1], (PREFIX, KV_HEADS, HEAD_DIM), jnp.float32).astype(jnp.bfloat16)
    value_act = jax.random.normal(part_keys[2], (PREFIX, KV_HEADS, HEAD_DIM), jnp.float32).astype(jnp.bfloat16)
    grad_dir = jax.random.normal(part_keys[3], q_shape, jnp.float32)
    out_noise = jax.random.normal(part_keys[4], q_shape, jnp.float32)
    out_grad = (GRAD_SCALE * grad_dir).astype(jnp.bfloat16)
    out_act = (0.125 * (grad_dir + out_noise)).astype(jnp.bfloat16)
    row_lse = forward_lse(query, key_act, doc_ids)
    return {'query': query, 'out_act': out_act, 'out_grad': out_grad, 'row_lse': row_lse, 'key_act': key_act, 'value_act': value_act, 'doc_ids': doc_ids}


def reference(query, out_act, out_grad, row_lse, key_act, value_act, doc_ids):
    n_blocks = SLICES * SPLITS
    blk_shape = (n_blocks, BLOCK_LEN, KV_HEADS, GROUP_SIZE, HEAD_DIM)
    key_f32 = key_act.astype(jnp.float32)
    value_f32 = value_act.astype(jnp.float32)
    xs_all = (query.reshape(blk_shape), out_act.reshape(blk_shape), out_grad.reshape(blk_shape), row_lse.reshape(n_blocks, BLOCK_LEN, KV_HEADS, GROUP_SIZE), PRE_LEN + jnp.arange(n_blocks) * BLOCK_LEN)

    def block_step(carry_in, xs_blk):
        dk_acc, dv_acc = carry_in
        q_blk, o_blk, do_blk, lse_blk, first_pos = xs_blk
        scores, allowed = masked_scores(q_blk, key_act, doc_ids, first_pos)
        p_full = jnp.where(allowed, jnp.exp(scores - lse_blk[..., None]), 0.0)
        p_half = p_full.astype(jnp.bfloat16).astype(jnp.float32)
        grad_f32 = do_blk.astype(jnp.float32)
        row_delta = jnp.sum(grad_f32 * o_blk.astype(jnp.float32), axis=-1)
        dv_acc = dv_acc + jnp.einsum('qhgk,qhgd->khd', p_half, grad_f32)
        d_prob = jnp.einsum('qhgd,khd->qhgk', grad_f32, value_f32)
        d_score = (p_full * (d_prob - row_delta[..., None])).astype(jnp.bfloat16).astype(jnp.float32)
        dq_blk = (jnp.einsum('qhgk,khd->qhgd', d_score, key_f32) * SCORE_SCALE).astype(jnp.bfloat16)
        dk_acc = dk_acc + jnp.einsum('qhgk,qhgd->khd', d_score, q_blk.astype(jnp.float32)) * SCORE_SCALE
        return (dk_acc, dv_acc), dq_blk

    zero_acc = jnp.zeros((PREFIX, KV_HEADS, HEAD_DIM), jnp.float32)
    (d_key, d_value), dq_blocks = lax.scan(block_step, (zero_acc, zero_acc), xs_all)
    return dq_blocks.reshape(SLICES, SUB_LEN, Q_HEADS, HEAD_DIM), d_key, d_value
```

```python
import functools
import math

import jax
import jax.numpy as jnp
from jax import lax
from jax.experimental import pallas as pl
from jax.experimental.pallas import tpu as pltpu
from jax.sharding import PartitionSpec as P

LOG2E = 1.4426950408889634
VMEM = pltpu.VMEM
NT = (((1,), (1,)), ((), ()))
NN = (((1,), (0,)), ((), ()))
TN = (((0,), (0,)), ((), ()))


def place(side):
    me = lax.axis_index('cp')
    return me // (2 * side), (me // 2) % side, me % 2


def rank_of(side, y, x, c):
    return {'cp': ((y % side) * side + (x % side)) * 2 + c}


def remote(src, dst, sems, i, to):
    return pltpu.make_async_remote_copy(
        src_ref=src, dst_ref=dst, send_sem=sems.at[0, i], recv_sem=sems.at[1, i],
        device_id=to, device_id_type=pl.DeviceIdType.MESH)


def greet(peers):
    barrier = pltpu.get_barrier_semaphore()
    for p in peers:
        pl.semaphore_signal(barrier, inc=1, device_id=p, device_id_type=pl.DeviceIdType.MESH)
    pl.semaphore_wait(barrier, len(peers))


def gather_kernel(side, qd, st, kv, qg, sg, kg, sx, sy, sp, ss, sl):
    y, x, c = place(side)
    right, left = rank_of(side, y, x + 1, c), rank_of(side, y, x + side - 1, c)
    far = rank_of(side, y, x + 2, c)
    up, down = rank_of(side, y + 1, x, c), rank_of(side, y + side - 1, x, c)
    mate = rank_of(side, y, x, 1 - c)
    xl, xr, xf = (x + side - 1) % side, (x + 1) % side, (x + 2) % side
    yl, yr, yf = (y + side - 1) % side, (y + 1) % side, (y + 2) % side
    greet((right, left, far, up, down, mate))

    ya = remote(kv.at[0], kg.at[y, 0, c], sy, 0, up)
    yc = remote(kv.at[1], kg.at[y, 1, c], sy, 2, down)
    xa = remote(qd.at[0], qg.at[x, 0], sx, 0, right)
    xc = remote(qd.at[1], qg.at[x, 1], sx, 2, left)
    yb = remote(kv.at[1], kg.at[y, 1, c], sy, 1, up)
    yd = remote(kv.at[0], kg.at[y, 0, c], sy, 3, down)
    xb = remote(qd.at[1], qg.at[x, 1], sx, 1, right)
    xd = remote(qd.at[0], qg.at[x, 0], sx, 3, left)
    s0 = remote(st, sg.at[x], ss, 0, right)
    s1 = remote(st, sg.at[x], ss, 1, left)
    s2 = remote(st, sg.at[x], ss, 2, far)
    p0 = remote(kv, kg.at[y, :, c], sp, 0, mate)
    sends = [s0, s1, s2, ya, yc, xa, xc, yb, yd, xb, xd, p0]
    for d in sends:
        d.start()
    own = [pltpu.make_async_copy(qd, qg.at[x], sl.at[0]),
           pltpu.make_async_copy(st, sg.at[x], sl.at[1]),
           pltpu.make_async_copy(kv, kg.at[y, :, c], sl.at[2])]
    for d in own:
        d.start()

    ya.wait_recv()
    ye = remote(kg.at[yl, 0, c], kg.at[yl, 0, c], sy, 4, up)
    ye.start()
    yc.wait_recv()
    yg = remote(kg.at[yr, 1, c], kg.at[yr, 1, c], sy, 5, down)
    yg.start()
    xa.wait_recv()
    xe = remote(qg.at[xl, 0], qg.at[xl, 0], sx, 4, right)
    xe.start()
    xc.wait_recv()
    xg = remote(qg.at[xr, 1], qg.at[xr, 1], sx, 5, left)
    xg.start()
    yb.wait_recv()
    p1 = remote(kg.at[yl, :, c], kg.at[yl, :, c], sp, 1, mate)
    p1.start()
    yd.wait_recv()
    p2 = remote(kg.at[yr, :, c], kg.at[yr, :, c], sp, 2, mate)
    p2.start()
    ye.wait_recv()
    yg.wait_recv()
    p3 = remote(kg.at[yf, :, c], kg.at[yf, :, c], sp, 3, mate)
    p3.start()
    for d in (xb, xd, xe, xg, s0, s1, s2, p0, p1, p2, p3):
        d.wait_recv()
    for d in own:
        d.wait()
    for d in sends + [ye, yg, xe, xg, p1, p2, p3]:
        d.wait_send()


def reduce_kernel(side, scale, chunk, dq, dkv, dq_out, dk_out, dv_out,
                  pc, acc, ka, kb, kt, qa, qb, qt, sx, sy, sp):
    y, x, c = place(side)
    right, left = rank_of(side, y, x + 1, c), rank_of(side, y, x + side - 1, c)
    up, down = rank_of(side, y + 1, x, c), rank_of(side, y + side - 1, x, c)
    mate = rank_of(side, y, x, 1 - c)
    xl, xr, xf = (x + side - 1) % side, (x + 1) % side, (x + 2) % side
    yl, yr, yf = (y + side - 1) % side, (y + 1) % side, (y + 2) % side
    half = dq.shape[1] // 2
    h0, h1 = pl.ds(0, half), pl.ds(half, half)
    greet((right, left, up, down, mate))

    def add(out, a, b):
        def step(i, _):
            rows = pl.ds(pl.multiple_of(i * chunk, chunk), chunk)
            out[rows, :] = a[rows, :] + b[rows, :]
            return 0
        lax.fori_loop(0, out.shape[0] // chunk, step, 0)

    slots = (yf, yr, yl, y)
    mates = [remote(dkv.at[s, :, 1 - c], pc.at[s], sp, i, mate) for i, s in enumerate(slots)]
    xa = remote(dq.at[xf, h0], qa.at[0], sx, 0, right)
    xc = remote(dq.at[xf, h1], qa.at[1], sx, 1, left)
    xb = remote(dq.at[xr, h1], qb.at[0, h1], sx, 2, right)
    xd = remote(dq.at[xl, h0], qb.at[1, h0], sx, 3, left)
    sends = [mates[0], xa, xc, mates[1], mates[2], mates[3], xb, xd]
    for d in sends:
        d.start()

    mates[0].wait_recv()
    for j in range(2):
        add(acc.at[yf, j], dkv.at[yf, j, c], pc.at[yf, j])
    ya = remote(acc.at[yf, 0], ka.at[0], sy, 0, up)
    yc = remote(acc.at[yf, 1], ka.at[1], sy, 1, down)
    ya.start()
    yc.start()
    mates[1].wait_recv()
    mates[2].wait_recv()
    add(acc.at[yr, 1], dkv.at[yr, 1, c], pc.at[yr, 1])
    yb = remote(acc.at[yr, 1], kb.at[0, 1], sy, 2, up)
    yb.start()
    add(acc.at[yl, 0], dkv.at[yl, 0, c], pc.at[yl, 0])
    yd = remote(acc.at[yl, 0], kb.at[1, 0], sy, 3, down)
    yd.start()
    add(acc.at[yr, 0], dkv.at[yr, 0, c], pc.at[yr, 0])
    add(acc.at[yl, 1], dkv.at[yl, 1, c], pc.at[yl, 1])
    mates[3].wait_recv()
    for j in range(2):
        add(acc.at[y, j], dkv.at[y, j, c], pc.at[y, j])

    xa.wait_recv()
    add(qt.at[0], dq.at[xr, h0], qa.at[0])
    xe = remote(qt.at[0], qb.at[0, h0], sx, 4, right)
    xe.start()
    xc.wait_recv()
    add(qt.at[1], dq.at[xl, h1], qa.at[1])
    xg = remote(qt.at[1], qb.at[1, h1], sx, 5, left)
    xg.start()
    ya.wait_recv()
    add(kt.at[0], acc.at[yr, 0], ka.at[0])
    ye = remote(kt.at[0], kb.at[0, 0], sy, 4, up)
    ye.start()
    yc.wait_recv()
    add(kt.at[1], acc.at[yl, 1], ka.at[1])
    yg = remote(kt.at[1], kb.at[1, 1], sy, 5, down)
    yg.start()

    for d in (xb, xd, xe, xg):
        d.wait_recv()

    def fin_q(i, _):
        rows = pl.ds(pl.multiple_of(i * chunk, chunk), chunk)
        total = dq[x, rows, :] + qb[0, rows, :] + qb[1, rows, :]
        dq_out[rows, :] = (total * scale).astype(dq_out.dtype)
        return 0

    lax.fori_loop(0, dq_out.shape[0] // chunk, fin_q, 0)
    for d in (yb, yd, ye, yg):
        d.wait_recv()

    def fin_k(i, _):
        rows = pl.ds(pl.multiple_of(i * chunk, chunk), chunk)
        dk_out[rows, :] = (acc[y, 0, rows, :] + kb[0, 0, rows, :] + kb[1, 0, rows, :]) * scale
        dv_out[rows, :] = acc[y, 1, rows, :] + kb[0, 1, rows, :] + kb[1, 1, rows, :]
        return 0

    lax.fori_loop(0, dk_out.shape[0] // chunk, fin_k, 0)
    for d in sends + [ya, yc, yb, yd, ye, yg, xe, xg]:
        d.wait_send()


def core_kernel(side, kt, sub_rows, span, sub_start, scale, bounds, qg, st, ids, kdoc, kg, dq, dkv, kcol):
    n_tiles = kg.shape[2] // kt
    rows_part = 2 * sub_rows
    tile_rows = side * rows_part
    lanes = 128
    dq[...] = jnp.zeros_like(dq)
    dkv[...] = jnp.zeros_like(dkv)

    def key_tile(t, _):
        yy, tt = t // n_tiles, t % n_tiles
        k0, hi = bounds[0, t], bounds[1, t]
        keys = pl.ds(pl.multiple_of(tt * kt, kt), kt)
        lo = jnp.maximum(k0 - sub_start, 0) // span

        @pl.when(hi > lo)
        def _():
            for g in range(kt // lanes):
                line = kdoc[t, pl.ds(g, 1), :]
                kcol[pl.ds(g * lanes, lanes), :] = jnp.broadcast_to(line, (lanes, lanes)).T

            def row_tile(i, _):
                part = pl.ds(pl.multiple_of(i * rows_part, rows_part), rows_part)
                k, v = kg[yy, 0, keys, :], kg[yy, 1, keys, :]
                q = jnp.concatenate([qg[s, 0, part, :] for s in range(side)], axis=0)
                do = jnp.concatenate([qg[s, 1, part, :] for s in range(side)], axis=0)
                lse, delta = st[i, pl.ds(0, 1), :], st[i, pl.ds(1, 1), :]
                qpos, qdoc = ids[i, pl.ds(0, 1), :], ids[i, pl.ds(1, 1), :]
                kd = jnp.concatenate([kcol[...]] * (tile_rows // lanes), axis=1)
                kpos = k0 + lax.broadcasted_iota(jnp.int32, (kt, tile_rows), 0)
                s_t = lax.dot_general(k, q, NT, preferred_element_type=jnp.float32)
                dp_t = lax.dot_general(v, do, NT, preferred_element_type=jnp.float32)
                p = jnp.exp2(s_t * (scale * LOG2E) - lse)
                p = jnp.where((kpos <= qpos) & (kd == qdoc), p, 0.0)
                ds = (p * (dp_t - delta)).astype(jnp.bfloat16)
                dkv[yy, 1, keys, :] += lax.dot_general(p.astype(jnp.bfloat16), do, NN, preferred_element_type=jnp.float32)
                dkv[yy, 0, keys, :] += lax.dot_general(ds, q, NN, preferred_element_type=jnp.float32)
                dq_t = lax.dot_general(ds, k, TN, preferred_element_type=jnp.float32)
                for s in range(side):
                    dq[s, part, :] += dq_t[s * rows_part:(s + 1) * rows_part, :]
                return 0

            lax.fori_loop(lo, hi, row_tile, 0)
        return 0

    lax.fori_loop(0, bounds.shape[1], key_tile, 0)


def solution(mesh):
    cp_size = mesh.shape['cp']
    side = math.isqrt(cp_size // 2)
    assert side == 4 and side * side * 2 == cp_size
    q_spec = P(None, 'cp', 'tp', None)
    lse_spec = P(None, 'cp', 'tp')
    kv_spec = P('cp', 'tp', None)
    vspec = pl.BlockSpec(memory_space=VMEM)
    dma = pltpu.SemaphoreType.DMA

    def local_backward(query, out_act, out_grad, row_lse, key_act, value_act, doc_ids):
        n_sub, local_len, n_heads, head_dim = query.shape
        keys_local, n_kv = key_act.shape[0], key_act.shape[1]
        assert n_kv == 1
        f32, bf16 = jnp.float32, jnp.bfloat16
        sub_len = local_len * cp_size
        n_keys = keys_local * cp_size
        sub_start = n_keys - n_sub * sub_len
        scale = head_dim ** -0.5
        sub_rows = local_len * n_heads
        rows = n_sub * sub_rows
        pair = 2 * keys_local
        kt = 512
        span = 2 * sub_len
        n_row_tiles = n_sub // 2
        per_y = pair // kt
        y, x, c = place(side)

        qd = jnp.stack([query.reshape(rows, head_dim), out_grad.reshape(rows, head_dim)])
        delta = jnp.sum(out_grad.astype(f32) * out_act.astype(f32), axis=-1)
        st = jnp.stack([row_lse.reshape(rows // 128, 128) * LOG2E, delta.reshape(rows // 128, 128)])
        kv = jnp.stack([key_act.reshape(keys_local, head_dim), value_act.reshape(keys_local, head_dim)])

        qg, sg, kg = pl.pallas_call(
            functools.partial(gather_kernel, side),
            out_shape=[jax.ShapeDtypeStruct((side,) + qd.shape, bf16),
                       jax.ShapeDtypeStruct((side,) + st.shape, f32),
                       jax.ShapeDtypeStruct((side, 2, 2, keys_local, head_dim), bf16)],
            in_specs=[vspec] * 3, out_specs=[vspec] * 3,
            scratch_shapes=[dma((2, 6)), dma((2, 6)), dma((2, 4)), dma((2, 3)), dma((3,))],
            compiler_params=pltpu.CompilerParams(collective_id=0, has_side_effects=True),
            name='gather')(qd, st, kv)

        st_rows = sg.reshape(side, 2, n_row_tiles, 2 * sub_rows).transpose(2, 1, 0, 3).reshape(n_row_tiles, 2, side * 2 * sub_rows)
        q_ids = doc_ids[sub_start:].reshape(n_row_tiles, 2, side, side, 2, local_len)
        q_ids = lax.dynamic_slice(q_ids, (0, 0, y, 0, c, 0), (n_row_tiles, 2, 1, side, 1, local_len)).reshape(n_row_tiles, 2, side, local_len)
        q_pos = (sub_start + jnp.arange(n_sub, dtype=jnp.int32).reshape(n_row_tiles, 2, 1, 1) * sub_len
                 + ((y * side + jnp.arange(side, dtype=jnp.int32)) * 2 + c).reshape(side, 1) * local_len
                 + jnp.arange(local_len, dtype=jnp.int32))
        ids = jnp.stack([q_pos, q_ids], axis=1).transpose(0, 1, 3, 2, 4)
        ids = jnp.broadcast_to(ids[..., None], ids.shape + (n_heads,)).reshape(n_row_tiles, 2, side * 2 * sub_rows)
        k_ids = lax.dynamic_slice(doc_ids.reshape(side, side, pair), (0, x, 0), (side, 1, pair))
        k_ids = k_ids.reshape(side * per_y, kt // 128, 128)
        k_first = (((jnp.arange(side, dtype=jnp.int32) * side + x) * pair).reshape(side, 1)
                   + jnp.arange(per_y, dtype=jnp.int32) * kt).reshape(-1)
        q_first = doc_ids[sub_start:].reshape(n_row_tiles, span)[:, 0]
        k_last = k_ids.reshape(side * per_y, kt)[:, -1]
        hi = jnp.sum((q_first[None, :] <= k_last[:, None]).astype(jnp.int32), axis=1)
        bounds = jnp.stack([k_first, hi])

        dq, dkv = pl.pallas_call(
            functools.partial(core_kernel, side, kt, sub_rows, span, sub_start, scale),
            out_shape=[jax.ShapeDtypeStruct((side, rows, head_dim), f32),
                       jax.ShapeDtypeStruct((side, 2, pair, head_dim), f32)],
            in_specs=[pl.BlockSpec(memory_space=pltpu.SMEM)] + [vspec] * 5, out_specs=[vspec] * 2,
            scratch_shapes=[VMEM((kt, 128), jnp.int32)],
            name='pairs')(bounds, qg, st_rows, ids, k_ids, kg.reshape(side, 2, pair, head_dim))

        half = rows // 2
        dq_out, dk, dv = pl.pallas_call(
            functools.partial(reduce_kernel, side, scale, 128),
            out_shape=[jax.ShapeDtypeStruct((rows, head_dim), bf16),
                       jax.ShapeDtypeStruct((keys_local, head_dim), f32),
                       jax.ShapeDtypeStruct((keys_local, head_dim), f32)],
            in_specs=[vspec] * 2, out_specs=[vspec] * 3,
            scratch_shapes=[VMEM((side, 2, keys_local, head_dim), f32), VMEM((side, 2, keys_local, head_dim), f32),
                            VMEM((2, keys_local, head_dim), f32), VMEM((2, 2, keys_local, head_dim), f32), VMEM((2, keys_local, head_dim), f32),
                            VMEM((2, half, head_dim), f32), VMEM((2, rows, head_dim), f32), VMEM((2, half, head_dim), f32),
                            dma((2, 6)), dma((2, 6)), dma((2, 4))],
            compiler_params=pltpu.CompilerParams(collective_id=1, has_side_effects=True),
            name='reduce')(dq, dkv.reshape(side, 2, 2, keys_local, head_dim))
        return dq_out.reshape(query.shape), dk.reshape(key_act.shape), dv.reshape(value_act.shape)

    return jax.shard_map(local_backward, mesh=mesh, in_specs=(q_spec, q_spec, q_spec, lse_spec, kv_spec, kv_spec, P()), out_specs=(q_spec, kv_spec, kv_spec), check_vma=False)
```

```python
import functools
import math

import jax
import jax.numpy as jnp
from jax import lax
from jax.experimental import pallas as pl
from jax.experimental.pallas import tpu as pltpu
from jax.sharding import PartitionSpec as P

LOG2E = 1.4426950408889634
VMEM = pltpu.VMEM
NT = (((1,), (1,)), ((), ()))
NN = (((1,), (0,)), ((), ()))
TN = (((0,), (0,)), ((), ()))


def place(side):
    me = lax.axis_index('cp')
    return me // (2 * side), (me // 2) % side, me % 2


def rank_of(side, y, x, c):
    return {'cp': ((y % side) * side + (x % side)) * 2 + c}


def remote(src, dst, sems, i, to):
    return pltpu.make_async_remote_copy(
        src_ref=src, dst_ref=dst, send_sem=sems.at[0, i], recv_sem=sems.at[1, i],
        device_id=to, device_id_type=pl.DeviceIdType.MESH)


def greet(peers):
    barrier = pltpu.get_barrier_semaphore()
    for p in peers:
        pl.semaphore_signal(barrier, inc=1, device_id=p, device_id_type=pl.DeviceIdType.MESH)
    pl.semaphore_wait(barrier, len(peers))


def doc_ends(doc):
    n_rows, lanes = doc.shape
    far = n_rows * lanes
    row = lax.broadcasted_iota(jnp.int32, doc.shape, 0)
    lane = lax.broadcasted_iota(jnp.int32, doc.shape, 1)
    pos = row * lanes + lane
    below = pltpu.roll(doc, n_rows - 1, 0)
    after = jnp.where(lane == lanes - 1, pltpu.roll(below, lanes - 1, 1), pltpu.roll(doc, lanes - 1, 1))
    end = jnp.where((doc != after) | (pos == far - 1), pos, far)
    s = 1
    while s < lanes:
        end = jnp.minimum(end, jnp.where(lane < lanes - s, pltpu.roll(end, lanes - s, 1), far))
        s *= 2
    first = jnp.broadcast_to(end[:, 0:1], doc.shape)
    later = jnp.where(row < n_rows - 1, pltpu.roll(first, n_rows - 1, 0), far)
    s = 1
    while s < n_rows:
        later = jnp.minimum(later, jnp.where(row < n_rows - s, pltpu.roll(later, n_rows - s, 0), far))
        s *= 2
    return jnp.minimum(end, later)


def gather_kernel(side, qdo, lse, kv, doc, qg, sg, kg, ends, st, sx, sy, sp, ss, sl):
    y, x, c = place(side)
    right, left = rank_of(side, y, x + 1, c), rank_of(side, y, x + side - 1, c)
    far = rank_of(side, y, x + 2, c)
    up, down = rank_of(side, y + 1, x, c), rank_of(side, y + side - 1, x, c)
    mate = rank_of(side, y, x, 1 - c)
    xl, xr, xf = (x + side - 1) % side, (x + 1) % side, (x + 2) % side
    yl, yr, yf = (y + side - 1) % side, (y + 1) % side, (y + 2) % side
    greet((right, left, far, up, down, mate))

    ya = remote(kv.at[0], kg.at[y, 0, c], sy, 0, up)
    yc = remote(kv.at[1], kg.at[y, 1, c], sy, 2, down)
    xa = remote(qdo.at[0], qg.at[x, 0], sx, 0, right)
    xc = remote(qdo.at[1], qg.at[x, 1], sx, 2, left)
    yb = remote(kv.at[1], kg.at[y, 1, c], sy, 1, up)
    yd = remote(kv.at[0], kg.at[y, 0, c], sy, 3, down)
    xb = remote(qdo.at[1], qg.at[x, 1], sx, 1, right)
    xd = remote(qdo.at[0], qg.at[x, 0], sx, 3, left)
    s0 = remote(st, sg.at[x], ss, 0, right)
    s1 = remote(st, sg.at[x], ss, 1, left)
    s2 = remote(st, sg.at[x], ss, 2, far)
    p0 = remote(kv, kg.at[y, :, c], sp, 0, mate)
    sends = [ya, yc, xa, xc, yb, yd, xb, xd, p0]
    for d in sends:
        d.start()
    own = [pltpu.make_async_copy(qdo.at[pl.ds(0, 2)], qg.at[x], sl.at[0]),
           pltpu.make_async_copy(kv, kg.at[y, :, c], sl.at[2]),
           pltpu.make_async_copy(st, sg.at[x], sl.at[1])]
    own[0].start()
    own[1].start()
    lanes = st.shape[-1]
    st[0] = lse[...] * LOG2E
    for g in range(st.shape[1]):
        rows = pl.ds(g * lanes, lanes)
        prod = qdo[1, rows, :].astype(jnp.float32) * qdo[2, rows, :].astype(jnp.float32)
        st[1, pl.ds(g, 1), :] = jnp.sum(prod.T, axis=0, keepdims=True)
    ends[...] = doc_ends(doc[...])

    ya.wait_recv()
    ye = remote(kg.at[yl, 0, c], kg.at[yl, 0, c], sy, 4, up)
    ye.start()
    yc.wait_recv()
    yg = remote(kg.at[yr, 1, c], kg.at[yr, 1, c], sy, 5, down)
    yg.start()
    own[2].start()
    for d in (s0, s1, s2):
        d.start()
    xa.wait_recv()
    xe = remote(qg.at[xl, 0], qg.at[xl, 0], sx, 4, right)
    xe.start()
    xc.wait_recv()
    xg = remote(qg.at[xr, 1], qg.at[xr, 1], sx, 5, left)
    xg.start()
    yb.wait_recv()
    p1 = remote(kg.at[yl, :, c], kg.at[yl, :, c], sp, 1, mate)
    p1.start()
    yd.wait_recv()
    p2 = remote(kg.at[yr, :, c], kg.at[yr, :, c], sp, 2, mate)
    p2.start()
    ye.wait_recv()
    yg.wait_recv()
    p3 = remote(kg.at[yf, :, c], kg.at[yf, :, c], sp, 3, mate)
    p3.start()
    for d in (xb, xd, xe, xg, s0, s1, s2, p0, p1, p2, p3):
        d.wait_recv()
    for d in own:
        d.wait()
    for d in sends + [s0, s1, s2, ye, yg, xe, xg, p1, p2, p3]:
        d.wait_send()


def reduce_kernel(side, scale, chunk, dq, dkv, dq_out, dk_out, dv_out,
                  pc, acc, ka, kb, kt, qa, qb, qt, sx, sy, sp):
    y, x, c = place(side)
    right, left = rank_of(side, y, x + 1, c), rank_of(side, y, x + side - 1, c)
    up, down = rank_of(side, y + 1, x, c), rank_of(side, y + side - 1, x, c)
    mate = rank_of(side, y, x, 1 - c)
    xl, xr, xf = (x + side - 1) % side, (x + 1) % side, (x + 2) % side
    yl, yr, yf = (y + side - 1) % side, (y + 1) % side, (y + 2) % side
    half = dq.shape[1] // 2
    h0, h1 = pl.ds(0, half), pl.ds(half, half)
    greet((right, left, up, down, mate))

    def add(out, a, b):
        def step(i, _):
            rows = pl.ds(pl.multiple_of(i * chunk, chunk), chunk)
            out[rows, :] = a[rows, :] + b[rows, :]
            return 0
        lax.fori_loop(0, out.shape[0] // chunk, step, 0)

    slots = (yf, yr, yl, y)
    mates = [remote(dkv.at[s, :, 1 - c], pc.at[s], sp, i, mate) for i, s in enumerate(slots)]
    xa = remote(dq.at[xf, h0], qa.at[0], sx, 0, right)
    xc = remote(dq.at[xf, h1], qa.at[1], sx, 1, left)
    xb = remote(dq.at[xr, h1], qb.at[0, h1], sx, 2, right)
    xd = remote(dq.at[xl, h0], qb.at[1, h0], sx, 3, left)
    sends = [mates[0], xa, xc, mates[1], mates[2], mates[3], xb, xd]
    for d in sends:
        d.start()

    mates[0].wait_recv()
    for j in range(2):
        add(acc.at[yf, j], dkv.at[yf, j, c], pc.at[yf, j])
    ya = remote(acc.at[yf, 0], ka.at[0], sy, 0, up)
    yc = remote(acc.at[yf, 1], ka.at[1], sy, 1, down)
    ya.start()
    yc.start()
    mates[1].wait_recv()
    mates[2].wait_recv()
    add(acc.at[yr, 1], dkv.at[yr, 1, c], pc.at[yr, 1])
    yb = remote(acc.at[yr, 1], kb.at[0, 1], sy, 2, up)
    yb.start()
    add(acc.at[yl, 0], dkv.at[yl, 0, c], pc.at[yl, 0])
    yd = remote(acc.at[yl, 0], kb.at[1, 0], sy, 3, down)
    yd.start()
    add(acc.at[yr, 0], dkv.at[yr, 0, c], pc.at[yr, 0])
    add(acc.at[yl, 1], dkv.at[yl, 1, c], pc.at[yl, 1])
    mates[3].wait_recv()
    for j in range(2):
        add(acc.at[y, j], dkv.at[y, j, c], pc.at[y, j])

    xa.wait_recv()
    add(qt.at[0], dq.at[xr, h0], qa.at[0])
    xe = remote(qt.at[0], qb.at[0, h0], sx, 4, right)
    xe.start()
    xc.wait_recv()
    add(qt.at[1], dq.at[xl, h1], qa.at[1])
    xg = remote(qt.at[1], qb.at[1, h1], sx, 5, left)
    xg.start()
    ya.wait_recv()
    add(kt.at[0], acc.at[yr, 0], ka.at[0])
    ye = remote(kt.at[0], kb.at[0, 0], sy, 4, up)
    ye.start()
    yc.wait_recv()
    add(kt.at[1], acc.at[yl, 1], ka.at[1])
    yg = remote(kt.at[1], kb.at[1, 1], sy, 5, down)
    yg.start()

    for d in (xb, xd, xe, xg):
        d.wait_recv()

    def fin_q(i, _):
        rows = pl.ds(pl.multiple_of(i * chunk, chunk), chunk)
        total = dq[x, rows, :] + qb[0, rows, :] + qb[1, rows, :]
        dq_out[rows, :] = (total * scale).astype(dq_out.dtype)
        return 0

    lax.fori_loop(0, dq_out.shape[0] // chunk, fin_q, 0)
    for d in (yb, yd, ye, yg):
        d.wait_recv()

    def fin_k(i, _):
        rows = pl.ds(pl.multiple_of(i * chunk, chunk), chunk)
        dk_out[rows, :] = (acc[y, 0, rows, :] + kb[0, 0, rows, :] + kb[1, 0, rows, :]) * scale
        dv_out[rows, :] = acc[y, 1, rows, :] + kb[0, 1, rows, :] + kb[1, 1, rows, :]
        return 0

    lax.fori_loop(0, dk_out.shape[0] // chunk, fin_k, 0)
    for d in sends + [ya, yc, yb, yd, ye, yg, xe, xg]:
        d.wait_send()


def reduce_upper_kernel(side, scale, chunk, n_part, dq, dkv, dq_out, dk_out, dv_out,
                        pc, acc, got, tot, end, qa, qb, qt, sx, sp, s1, s2):
    y, x, c = place(side)
    right, left = rank_of(side, y, x + 1, c), rank_of(side, y, x + side - 1, c)
    up, down = rank_of(side, y + 1, x, c), rank_of(side, y + side - 1, x, c)
    mate = rank_of(side, y, x, 1 - c)
    beside = rank_of(side, y + 1 - 2 * (y % 2), x, c)
    across = rank_of(side, side - 1 - y, x, c)
    xl, xr, xf = (x + side - 1) % side, (x + 1) % side, (x + 2) % side
    give = side // 2 + (y + y // 2) % 2
    keep = side + 1 - give
    lower = y < side // 2
    half = dq.shape[1] // 2
    h0, h1 = pl.ds(0, half), pl.ds(half, half)
    per = dkv.shape[3] // (n_part // 2)
    parts = [(i % 2, pl.ds((i // 2) * per, per)) for i in range(n_part)]
    greet((right, left, up, down, mate))

    def add(out, a, b):
        def step(i, _):
            rows = pl.ds(pl.multiple_of(i * chunk, chunk), chunk)
            out[rows, :] = a[rows, :] + b[rows, :]
            return 0
        lax.fori_loop(0, out.shape[0] // chunk, step, 0)

    m1 = [remote(dkv.at[give, j, 1 - c, r], pc.at[0, j, r], sp, i, mate) for i, (j, r) in enumerate(parts)]
    m2 = [remote(dkv.at[keep, j, 1 - c, r], pc.at[1, j, r], sp, n_part + i, mate) for i, (j, r) in enumerate(parts)]
    xa = remote(dq.at[xf, h0], qa.at[0], sx, 0, right)
    xc = remote(dq.at[xf, h1], qa.at[1], sx, 1, left)
    xb = remote(dq.at[xr, h1], qb.at[0, h1], sx, 2, right)
    xd = remote(dq.at[xl, h0], qb.at[1, h0], sx, 3, left)
    sends = m1 + [xa, xc] + m2 + [xb, xd]
    for d in sends:
        d.start()

    k1 = [remote(acc.at[0, j, r], got.at[j, r], s1, i, beside) for i, (j, r) in enumerate(parts)]
    k2 = [remote(tot.at[j, r], end.at[j, r], s2, i, across) for i, (j, r) in enumerate(parts)]
    for i, (j, r) in enumerate(parts):
        m1[i].wait_recv()
        acc[0, j, r, :] = dkv[give, j, c, r, :] + pc[0, j, r, :]
        k1[i].start()
    for i, (j, r) in enumerate(parts):
        m2[i].wait_recv()
        acc[1, j, r, :] = dkv[keep, j, c, r, :] + pc[1, j, r, :]
    for i, (j, r) in enumerate(parts):
        k1[i].wait_recv()
        tot[j, r, :] = acc[1, j, r, :] + got[j, r, :]

        @pl.when(lower)
        def _():
            k2[i].start()

        if i == 1:
            xa.wait_recv()
            add(qt.at[0], dq.at[xr, h0], qa.at[0])
            xe = remote(qt.at[0], qb.at[0, h0], sx, 4, right)
            xe.start()
            xc.wait_recv()
            add(qt.at[1], dq.at[xl, h1], qa.at[1])
            xg = remote(qt.at[1], qb.at[1, h1], sx, 5, left)
            xg.start()

    for d in (xb, xd, xe, xg):
        d.wait_recv()

    def fin_q(i, _):
        rows = pl.ds(pl.multiple_of(i * chunk, chunk), chunk)
        total = dq[x, rows, :] + qb[0, rows, :] + qb[1, rows, :]
        dq_out[rows, :] = (total * scale).astype(dq_out.dtype)
        return 0

    lax.fori_loop(0, dq_out.shape[0] // chunk, fin_q, 0)

    @pl.when(jnp.logical_not(lower))
    def _():
        for i, (j, r) in enumerate(parts):
            k2[i].wait_recv()
            if j == 0:
                dk_out[r, :] = (tot[j, r, :] + end[j, r, :]) * scale
            else:
                dv_out[r, :] = tot[j, r, :] + end[j, r, :]

    @pl.when(lower)
    def _():
        dk_out[...] = jnp.zeros_like(dk_out)
        dv_out[...] = jnp.zeros_like(dv_out)
        for d in k2:
            d.wait_send()

    for d in sends + k1 + [xe, xg]:
        d.wait_send()


def core_kernel(side, kt, sub_len, local_len, n_heads, sub_start, scale, first_y, ends, qg, sg, kg, dq, dkv, kcol, pbuf0, pbuf1, sbuf0, sbuf1, stat):
    pbuf, sbuf = (pbuf0, pbuf1), (sbuf0, sbuf1)
    y, x, c = place(side)
    pair = kg.shape[2]
    n_tiles = pair // kt
    sub_rows = local_len * n_heads
    rows_part = 2 * sub_rows
    tile_rows = side * rows_part
    span = 2 * sub_len
    lanes = 128
    dq[...] = jnp.zeros_like(dq)
    for yy in range(first_y, side):
        dkv[yy] = jnp.zeros(dkv.shape[1:], dkv.dtype)
    per_line = lanes // rows_part
    low = lax.broadcasted_iota(jnp.int32, (stat.shape[2], lanes), 1) < rows_part
    for j in range(2):
        for h in range(side // per_line):
            u, w = sg[2 * h, j], sg[2 * h + 1, j]
            at = pl.ds(h * lanes, lanes)
            stat[j, 0, :, at] = jnp.where(low, u, pltpu.roll(w, rows_part, 1))
            stat[j, 1, :, at] = jnp.where(low, pltpu.roll(u, rows_part, 1), w)
    spot = lax.broadcasted_iota(jnp.int32, (1, tile_rows), 1)
    qpos0 = (sub_start + ((spot // sub_rows) % 2) * sub_len + (spot // n_heads) % local_len
             + ((y * side + spot // rows_part) * 2 + c) * local_len)

    def key_tile(t, _):
        yy, tt = lax.div(t, n_tiles), lax.rem(t, n_tiles)
        k0 = (yy * side + x) * pair + tt * kt
        line0 = lax.div(k0, lanes)
        keys = pl.ds(pl.multiple_of(tt * kt, kt), kt)
        lo = lax.div(jnp.maximum(k0 - sub_start, 0), span)
        last = jnp.max(ends[pl.ds(line0 + kt // lanes - 1, 1), :])
        hi = lax.div(jnp.maximum(last - sub_start + span, 0), span)

        @pl.when(hi > lo)
        def _():
            for g in range(kt // lanes):
                line = ends[pl.ds(line0 + g, 1), :]
                kcol[pl.ds(g * lanes, lanes), :] = jnp.broadcast_to(line, (lanes, lanes)).T

            def operands(i):
                part = pl.ds(pl.multiple_of(i * rows_part, rows_part), rows_part)
                q = jnp.concatenate([qg[s, 0, part, :] for s in range(side)], axis=0)
                do = jnp.concatenate([qg[s, 1, part, :] for s in range(side)], axis=0)
                return part, q, do

            def weigh(i, b):
                part, q, do = operands(i)
                g, odd = lax.div(i, 2), lax.rem(i, 2)
                k, v = kg[yy, 0, keys, :], kg[yy, 1, keys, :]
                lse, delta = stat[0, odd, pl.ds(g, 1), :], stat[1, odd, pl.ds(g, 1), :]
                qpos = qpos0 + i * span
                kend = jnp.concatenate([kcol[...]] * (tile_rows // lanes), axis=1)
                kpos = k0 + lax.broadcasted_iota(jnp.int32, (kt, tile_rows), 0)
                s_t = lax.dot_general(k, q, NT, preferred_element_type=jnp.float32)
                dp_t = lax.dot_general(v, do, NT, preferred_element_type=jnp.float32)
                p = jnp.exp2(s_t * (scale * LOG2E) - lse)
                p = jnp.where((kpos <= qpos) & (qpos <= kend), p, 0.0)
                pbuf[b][...] = p.astype(jnp.bfloat16)
                sbuf[b][...] = (p * (dp_t - delta)).astype(jnp.bfloat16)

            def spread(i, b):
                part, q, do = operands(i)
                ds = sbuf[b][...]
                dkv[yy, 1, keys, :] += lax.dot_general(pbuf[b][...], do, NN, preferred_element_type=jnp.float32)
                dkv[yy, 0, keys, :] += lax.dot_general(ds, q, NN, preferred_element_type=jnp.float32)
                dq_t = lax.dot_general(ds, kg[yy, 0, keys, :], TN, preferred_element_type=jnp.float32)
                for s in range(side):
                    dq[s, part, :] += dq_t[s * rows_part:(s + 1) * rows_part, :]

            weigh(lo, 0)

            def two_tiles(m, _):
                i = lo + 1 + 2 * m
                weigh(i, 1)
                spread(i - 1, 0)
                weigh(i + 1, 0)
                spread(i, 1)
                return 0

            n_twos = lax.div(hi - lo - 1, 2)
            lax.fori_loop(0, n_twos, two_tiles, 0)
            even = hi - lo - 1 > 2 * n_twos

            @pl.when(even)
            def _():
                weigh(hi - 1, 1)
                spread(hi - 2, 0)
                spread(hi - 1, 1)

            @pl.when(jnp.logical_not(even))
            def _():
                spread(hi - 1, 0)
        return 0

    lax.fori_loop(first_y * n_tiles, side * n_tiles, key_tile, 0)


def solution(mesh):
    cp_size = mesh.shape['cp']
    side = math.isqrt(cp_size // 2)
    assert side == 4 and side * side * 2 == cp_size
    q_spec = P(None, 'cp', 'tp', None)
    lse_spec = P(None, 'cp', 'tp')
    kv_spec = P('cp', 'tp', None)
    vspec = pl.BlockSpec(memory_space=VMEM)
    dma = pltpu.SemaphoreType.DMA

    def local_backward(query, out_act, out_grad, row_lse, key_act, value_act, doc_ids):
        n_sub, local_len, n_heads, head_dim = query.shape
        keys_local, n_kv = key_act.shape[0], key_act.shape[1]
        assert n_kv == 1
        f32, bf16 = jnp.float32, jnp.bfloat16
        sub_len = local_len * cp_size
        n_keys = keys_local * cp_size
        sub_start = n_keys - n_sub * sub_len
        scale = head_dim ** -0.5
        sub_rows = local_len * n_heads
        rows = n_sub * sub_rows
        pair = 2 * keys_local
        kt = 768
        lanes = 128
        st_shape = (2, rows // lanes, lanes)
        half = rows // 2
        n_part = 8
        kv_shape = (2, keys_local, head_dim)
        q_scratch = [VMEM((2, half, head_dim), f32), VMEM((2, rows, head_dim), f32), VMEM((2, half, head_dim), f32), dma((2, 6))]

        def run(first_y, ident, qdo, lse, kv, doc):
            qg, sg, kg, ends = pl.pallas_call(
                functools.partial(gather_kernel, side),
                out_shape=[jax.ShapeDtypeStruct((side, 2, rows, head_dim), bf16),
                           jax.ShapeDtypeStruct((side,) + st_shape, f32),
                           jax.ShapeDtypeStruct((side, 2, 2, keys_local, head_dim), bf16),
                           jax.ShapeDtypeStruct(doc.shape, jnp.int32)],
                in_specs=[vspec] * 4, out_specs=[vspec] * 4,
                scratch_shapes=[VMEM(st_shape, f32), dma((2, 6)), dma((2, 6)), dma((2, 4)), dma((2, 3)), dma((3,))],
                compiler_params=pltpu.CompilerParams(collective_id=ident, has_side_effects=True, vmem_limit_bytes=24 << 20),
                name='gather')(qdo, lse, kv, doc)

            tile_rows = side * 2 * sub_rows
            dq, dkv = pl.pallas_call(
                functools.partial(core_kernel, side, kt, sub_len, local_len, n_heads, sub_start, scale, first_y),
                out_shape=[jax.ShapeDtypeStruct((side, rows, head_dim), f32),
                           jax.ShapeDtypeStruct((side, 2, pair, head_dim), f32)],
                in_specs=[vspec] * 4, out_specs=[vspec] * 2,
                scratch_shapes=[VMEM((kt, lanes), jnp.int32), *[VMEM((kt, tile_rows), bf16)] * 4,
                                VMEM((2, 2, rows // lanes, tile_rows), f32)],
                compiler_params=pltpu.CompilerParams(vmem_limit_bytes=30 << 20),
                name='pairs')(ends, qg, sg, kg.reshape(side, 2, pair, head_dim))

            if first_y:
                body = functools.partial(reduce_upper_kernel, side, scale, 128, n_part)
                scratch = [VMEM((2,) + kv_shape, f32), VMEM((2,) + kv_shape, f32), *[VMEM(kv_shape, f32)] * 3,
                           *q_scratch, dma((2, 2 * n_part)), dma((2, n_part)), dma((2, n_part))]
            else:
                body = functools.partial(reduce_kernel, side, scale, 128)
                scratch = [VMEM((side,) + kv_shape, f32), VMEM((side,) + kv_shape, f32), VMEM(kv_shape, f32),
                           VMEM((2,) + kv_shape, f32), VMEM(kv_shape, f32), *q_scratch, dma((2, 6)), dma((2, 4))]
            return pl.pallas_call(
                body,
                out_shape=[jax.ShapeDtypeStruct((rows, head_dim), bf16),
                           jax.ShapeDtypeStruct((keys_local, head_dim), f32),
                           jax.ShapeDtypeStruct((keys_local, head_dim), f32)],
                in_specs=[vspec] * 2, out_specs=[vspec] * 3, scratch_shapes=scratch,
                compiler_params=pltpu.CompilerParams(collective_id=ident + 1, has_side_effects=True, vmem_limit_bytes=30 << 20),
                name='reduce')(dq, dkv.reshape(side, 2, 2, keys_local, head_dim))

        qdo = jnp.stack([t.reshape(rows, head_dim) for t in (query, out_grad, out_act)])
        kv = jnp.stack([key_act.reshape(keys_local, head_dim), value_act.reshape(keys_local, head_dim)])
        upper = side // 2
        recent = doc_ids[upper * side * pair - 1] != doc_ids[sub_start]
        dq_out, dk, dv = lax.cond(recent, functools.partial(run, upper, 0), functools.partial(run, 0, 2),
                                  qdo, row_lse.reshape(rows // lanes, lanes), kv, doc_ids.reshape(n_keys // lanes, lanes))
        return dq_out.reshape(query.shape), dk.reshape(key_act.shape), dv.reshape(value_act.shape)

    return jax.shard_map(local_backward, mesh=mesh, in_specs=(q_spec, q_spec, q_spec, lse_spec, kv_spec, kv_spec, P()), out_specs=(q_spec, kv_spec, kv_spec), check_vma=False)
```

```python
import functools
import math

import jax
import jax.numpy as jnp
from jax import lax
from jax.experimental import pallas as pl
from jax.experimental.pallas import tpu as pltpu
from jax.sharding import PartitionSpec as P

LOG2E = 1.4426950408889634
VMEM = pltpu.VMEM
NT = (((1,), (1,)), ((), ()))
NN = (((1,), (0,)), ((), ()))
TN = (((0,), (0,)), ((), ()))


def place(side):
    me = lax.axis_index('cp')
    return me // (2 * side), (me // 2) % side, me % 2


def rank_of(side, y, x, c):
    return {'cp': ((y % side) * side + (x % side)) * 2 + c}


def remote(src, dst, sems, i, to):
    return pltpu.make_async_remote_copy(
        src_ref=src, dst_ref=dst, send_sem=sems.at[0, i], recv_sem=sems.at[1, i],
        device_id=to, device_id_type=pl.DeviceIdType.MESH)


def greet(peers):
    barrier = pltpu.get_barrier_semaphore()
    for p in peers:
        pl.semaphore_signal(barrier, inc=1, device_id=p, device_id_type=pl.DeviceIdType.MESH)
    pl.semaphore_wait(barrier, len(peers))


def doc_ends(doc):
    n_rows, lanes = doc.shape
    far = n_rows * lanes
    row = lax.broadcasted_iota(jnp.int32, doc.shape, 0)
    lane = lax.broadcasted_iota(jnp.int32, doc.shape, 1)
    pos = row * lanes + lane
    below = pltpu.roll(doc, n_rows - 1, 0)
    after = jnp.where(lane == lanes - 1, pltpu.roll(below, lanes - 1, 1), pltpu.roll(doc, lanes - 1, 1))
    end = jnp.where((doc != after) | (pos == far - 1), pos, far)
    s = 1
    while s < lanes:
        end = jnp.minimum(end, jnp.where(lane < lanes - s, pltpu.roll(end, lanes - s, 1), far))
        s *= 2
    first = jnp.broadcast_to(end[:, 0:1], doc.shape)
    later = jnp.where(row < n_rows - 1, pltpu.roll(first, n_rows - 1, 0), far)
    s = 1
    while s < n_rows:
        later = jnp.minimum(later, jnp.where(row < n_rows - s, pltpu.roll(later, n_rows - s, 0), far))
        s *= 2
    return jnp.minimum(end, later)


def gather_kernel(side, q, do, out, lse, k, v, doc, qg, sg, kg, ends, st, flip, sx, sy, sp, ss, sl):
    y, x, c = place(side)
    right, left = rank_of(side, y, x + 1, c), rank_of(side, y, x + side - 1, c)
    far = rank_of(side, y, x + 2, c)
    up, down = rank_of(side, y + 1, x, c), rank_of(side, y + side - 1, x, c)
    mate = rank_of(side, y, x, 1 - c)
    xl, xr, xf = (x + side - 1) % side, (x + 1) % side, (x + 2) % side
    yl, yr, yf = (y + side - 1) % side, (y + 1) % side, (y + 2) % side
    greet((right, left, far, up, down, mate))

    ya = remote(k, kg.at[y, 0, c], sy, 0, up)
    yc = remote(v, kg.at[y, 1, c], sy, 2, down)
    xa = remote(q, qg.at[x, 0], sx, 0, right)
    xc = remote(do, qg.at[x, 1], sx, 2, left)
    yb = remote(v, kg.at[y, 1, c], sy, 1, up)
    yd = remote(k, kg.at[y, 0, c], sy, 3, down)
    xb = remote(do, qg.at[x, 1], sx, 1, right)
    xd = remote(q, qg.at[x, 0], sx, 3, left)
    s0 = remote(st, sg.at[x], ss, 0, right)
    s1 = remote(st, sg.at[x], ss, 1, left)
    s2 = remote(st, sg.at[x], ss, 2, far)
    p0 = remote(k, kg.at[y, 0, c], sp, 0, mate)
    p4 = remote(v, kg.at[y, 1, c], sp, 4, mate)
    sends = [ya, yc, xa, xc, yb, yd, xb, xd, p0, p4]
    for d in sends:
        d.start()
    own = [pltpu.make_async_copy(q, qg.at[x, 0], sl.at[0]), pltpu.make_async_copy(do, qg.at[x, 1], sl.at[1]),
           pltpu.make_async_copy(k, kg.at[y, 0, c], sl.at[2]), pltpu.make_async_copy(v, kg.at[y, 1, c], sl.at[3]),
           pltpu.make_async_copy(st, sg.at[x], sl.at[4])]
    for d in own[:4]:
        d.start()
    lanes = st.shape[-1]
    sub_rows, n_sub = lse.shape
    flip[...] = jnp.zeros_like(flip)
    flip[pl.ds(0, sub_rows), pl.ds(0, n_sub)] = lse[...] * LOG2E
    flip[...] = flip[...].T
    folds = lanes // sub_rows
    lane = lax.broadcasted_iota(jnp.int32, (st.shape[1], lanes), 1)
    row_lse = jnp.zeros((st.shape[1], lanes), jnp.float32)
    for a in range(folds):
        some = flip[pl.ds(a, st.shape[1], stride=folds), :]
        some = pltpu.roll(some, a * sub_rows, 1) if a else some
        row_lse = jnp.where(lane // sub_rows == a, some, row_lse)
    st[0] = row_lse
    for g in range(st.shape[1]):
        rows = pl.ds(g * lanes, lanes)
        prod = do[rows, :].astype(jnp.float32) * out[rows, :].astype(jnp.float32)
        st[1, pl.ds(g, 1), :] = jnp.sum(prod.T, axis=0, keepdims=True)
    ends[...] = doc_ends(doc[...])

    ya.wait_recv()
    ye = remote(kg.at[yl, 0, c], kg.at[yl, 0, c], sy, 4, up)
    ye.start()
    yc.wait_recv()
    yg = remote(kg.at[yr, 1, c], kg.at[yr, 1, c], sy, 5, down)
    yg.start()
    own[4].start()
    for d in (s0, s1, s2):
        d.start()
    xa.wait_recv()
    xe = remote(qg.at[xl, 0], qg.at[xl, 0], sx, 4, right)
    xe.start()
    xc.wait_recv()
    xg = remote(qg.at[xr, 1], qg.at[xr, 1], sx, 5, left)
    xg.start()
    yb.wait_recv()
    p1 = remote(kg.at[yl, :, c], kg.at[yl, :, c], sp, 1, mate)
    p1.start()
    yd.wait_recv()
    p2 = remote(kg.at[yr, :, c], kg.at[yr, :, c], sp, 2, mate)
    p2.start()
    ye.wait_recv()
    yg.wait_recv()
    p3 = remote(kg.at[yf, :, c], kg.at[yf, :, c], sp, 3, mate)
    p3.start()
    for d in (xb, xd, xe, xg, s0, s1, s2, p0, p1, p2, p3, p4):
        d.wait_recv()
    for d in own:
        d.wait()
    for d in sends + [s0, s1, s2, ye, yg, xe, xg, p1, p2, p3]:
        d.wait_send()


def reduce_kernel(side, scale, chunk, dq, dkv, dq_out, dk_out, dv_out,
                  pc, acc, ka, kb, kt, qa, qb, qt, sx, sy, sp):
    y, x, c = place(side)
    right, left = rank_of(side, y, x + 1, c), rank_of(side, y, x + side - 1, c)
    up, down = rank_of(side, y + 1, x, c), rank_of(side, y + side - 1, x, c)
    mate = rank_of(side, y, x, 1 - c)
    xl, xr, xf = (x + side - 1) % side, (x + 1) % side, (x + 2) % side
    yl, yr, yf = (y + side - 1) % side, (y + 1) % side, (y + 2) % side
    half = dq.shape[1] // 2
    h0, h1 = pl.ds(0, half), pl.ds(half, half)
    greet((right, left, up, down, mate))

    def add(out, a, b):
        def step(i, _):
            rows = pl.ds(pl.multiple_of(i * chunk, chunk), chunk)
            out[rows, :] = a[rows, :] + b[rows, :]
            return 0
        lax.fori_loop(0, out.shape[0] // chunk, step, 0)

    slots = (yf, yr, yl, y)
    mates = [remote(dkv.at[s, :, 1 - c], pc.at[s], sp, i, mate) for i, s in enumerate(slots)]
    xa = remote(dq.at[xf, h0], qa.at[0], sx, 0, right)
    xc = remote(dq.at[xf, h1], qa.at[1], sx, 1, left)
    xb = remote(dq.at[xr, h1], qb.at[0, h1], sx, 2, right)
    xd = remote(dq.at[xl, h0], qb.at[1, h0], sx, 3, left)
    sends = [mates[0], xa, xc, mates[1], mates[2], mates[3], xb, xd]
    for d in sends:
        d.start()

    mates[0].wait_recv()
    for j in range(2):
        add(acc.at[yf, j], dkv.at[yf, j, c], pc.at[yf, j])
    ya = remote(acc.at[yf, 0], ka.at[0], sy, 0, up)
    yc = remote(acc.at[yf, 1], ka.at[1], sy, 1, down)
    ya.start()
    yc.start()
    mates[1].wait_recv()
    mates[2].wait_recv()
    add(acc.at[yr, 1], dkv.at[yr, 1, c], pc.at[yr, 1])
    yb = remote(acc.at[yr, 1], kb.at[0, 1], sy, 2, up)
    yb.start()
    add(acc.at[yl, 0], dkv.at[yl, 0, c], pc.at[yl, 0])
    yd = remote(acc.at[yl, 0], kb.at[1, 0], sy, 3, down)
    yd.start()
    add(acc.at[yr, 0], dkv.at[yr, 0, c], pc.at[yr, 0])
    add(acc.at[yl, 1], dkv.at[yl, 1, c], pc.at[yl, 1])
    mates[3].wait_recv()
    for j in range(2):
        add(acc.at[y, j], dkv.at[y, j, c], pc.at[y, j])

    xa.wait_recv()
    add(qt.at[0], dq.at[xr, h0], qa.at[0])
    xe = remote(qt.at[0], qb.at[0, h0], sx, 4, right)
    xe.start()
    xc.wait_recv()
    add(qt.at[1], dq.at[xl, h1], qa.at[1])
    xg = remote(qt.at[1], qb.at[1, h1], sx, 5, left)
    xg.start()
    ya.wait_recv()
    add(kt.at[0], acc.at[yr, 0], ka.at[0])
    ye = remote(kt.at[0], kb.at[0, 0], sy, 4, up)
    ye.start()
    yc.wait_recv()
    add(kt.at[1], acc.at[yl, 1], ka.at[1])
    yg = remote(kt.at[1], kb.at[1, 1], sy, 5, down)
    yg.start()

    for d in (xb, xd, xe, xg):
        d.wait_recv()

    def fin_q(i, _):
        rows = pl.ds(pl.multiple_of(i * chunk, chunk), chunk)
        total = dq[x, rows, :] + qb[0, rows, :] + qb[1, rows, :]
        dq_out[rows, :] = (total * scale).astype(dq_out.dtype)
        return 0

    lax.fori_loop(0, dq_out.shape[0] // chunk, fin_q, 0)
    for d in (yb, yd, ye, yg):
        d.wait_recv()

    def fin_k(i, _):
        rows = pl.ds(pl.multiple_of(i * chunk, chunk), chunk)
        dk_out[rows, :] = (acc[y, 0, rows, :] + kb[0, 0, rows, :] + kb[1, 0, rows, :]) * scale
        dv_out[rows, :] = acc[y, 1, rows, :] + kb[0, 1, rows, :] + kb[1, 1, rows, :]
        return 0

    lax.fori_loop(0, dk_out.shape[0] // chunk, fin_k, 0)
    for d in sends + [ya, yc, yb, yd, ye, yg, xe, xg]:
        d.wait_send()


def reduce_upper_kernel(side, scale, chunk, n_part, dq, dkv, dq_out, dk_out, dv_out,
                        pc, acc, got, tot, end, qa, qb, qt, sx, sp, s1, s2):
    y, x, c = place(side)
    right, left = rank_of(side, y, x + 1, c), rank_of(side, y, x + side - 1, c)
    up, down = rank_of(side, y + 1, x, c), rank_of(side, y + side - 1, x, c)
    mate = rank_of(side, y, x, 1 - c)
    beside = rank_of(side, y + 1 - 2 * (y % 2), x, c)
    across = rank_of(side, side - 1 - y, x, c)
    xl, xr, xf = (x + side - 1) % side, (x + 1) % side, (x + 2) % side
    give = side // 2 + (y + y // 2) % 2
    keep = side + 1 - give
    lower = y < side // 2
    half = dq.shape[1] // 2
    h0, h1 = pl.ds(0, half), pl.ds(half, half)
    per = dkv.shape[3] // (n_part // 2)
    parts = [(i % 2, pl.ds((i // 2) * per, per)) for i in range(n_part)]
    greet((right, left, up, down, mate))

    def add(out, a, b):
        def step(i, _):
            rows = pl.ds(pl.multiple_of(i * chunk, chunk), chunk)
            out[rows, :] = a[rows, :] + b[rows, :]
            return 0
        lax.fori_loop(0, out.shape[0] // chunk, step, 0)

    m1 = [remote(dkv.at[give, j, 1 - c, r], pc.at[0, j, r], sp, i, mate) for i, (j, r) in enumerate(parts)]
    m2 = [remote(dkv.at[keep, j, 1 - c, r], pc.at[1, j, r], sp, n_part + i, mate) for i, (j, r) in enumerate(parts)]
    xa = remote(dq.at[xf, h0], qa.at[0], sx, 0, right)
    xc = remote(dq.at[xf, h1], qa.at[1], sx, 1, left)
    xb = remote(dq.at[xr, h1], qb.at[0, h1], sx, 2, right)
    xd = remote(dq.at[xl, h0], qb.at[1, h0], sx, 3, left)
    sends = m1 + [xa, xc] + m2 + [xb, xd]
    for d in sends:
        d.start()

    k1 = [remote(acc.at[0, j, r], got.at[j, r], s1, i, beside) for i, (j, r) in enumerate(parts)]
    k2 = [remote(tot.at[j, r], end.at[j, r], s2, i, across) for i, (j, r) in enumerate(parts)]
    for i, (j, r) in enumerate(parts):
        m1[i].wait_recv()
        acc[0, j, r, :] = dkv[give, j, c, r, :] + pc[0, j, r, :]
        k1[i].start()
    for i, (j, r) in enumerate(parts):
        m2[i].wait_recv()
        acc[1, j, r, :] = dkv[keep, j, c, r, :] + pc[1, j, r, :]
    for i, (j, r) in enumerate(parts):
        k1[i].wait_recv()
        tot[j, r, :] = acc[1, j, r, :] + got[j, r, :]

        @pl.when(lower)
        def _():
            k2[i].start()

        if i == 1:
            xa.wait_recv()
            add(qt.at[0], dq.at[xr, h0], qa.at[0])
            xe = remote(qt.at[0], qb.at[0, h0], sx, 4, right)
            xe.start()
            xc.wait_recv()
            add(qt.at[1], dq.at[xl, h1], qa.at[1])
            xg = remote(qt.at[1], qb.at[1, h1], sx, 5, left)
            xg.start()

    for d in (xb, xd, xe, xg):
        d.wait_recv()

    def fin_q(i, _):
        rows = pl.ds(pl.multiple_of(i * chunk, chunk), chunk)
        total = dq[x, rows, :] + qb[0, rows, :] + qb[1, rows, :]
        dq_out[rows, :] = (total * scale).astype(dq_out.dtype)
        return 0

    lax.fori_loop(0, dq_out.shape[0] // chunk, fin_q, 0)

    @pl.when(jnp.logical_not(lower))
    def _():
        for i, (j, r) in enumerate(parts):
            k2[i].wait_recv()
            if j == 0:
                dk_out[r, :] = (tot[j, r, :] + end[j, r, :]) * scale
            else:
                dv_out[r, :] = tot[j, r, :] + end[j, r, :]

    @pl.when(lower)
    def _():
        dk_out[...] = jnp.zeros_like(dk_out)
        dv_out[...] = jnp.zeros_like(dv_out)
        for d in k2:
            d.wait_send()

    for d in sends + k1 + [xe, xg]:
        d.wait_send()


def core_kernel(side, kt, sub_len, local_len, n_heads, sub_start, scale, first_y, ends, qg, sg, kg, dq, dkv, kcol, pbuf0, pbuf1, sbuf0, sbuf1, stat):
    pbuf, sbuf = (pbuf0, pbuf1), (sbuf0, sbuf1)
    y, x, c = place(side)
    pair = kg.shape[2]
    n_tiles = pair // kt
    sub_rows = local_len * n_heads
    rows_part = 2 * sub_rows
    tile_rows = side * rows_part
    span = 2 * sub_len
    lanes = 128
    dq[...] = jnp.zeros_like(dq)
    for yy in range(first_y, side):
        dkv[yy] = jnp.zeros(dkv.shape[1:], dkv.dtype)
    per_line = lanes // rows_part
    low = lax.broadcasted_iota(jnp.int32, (stat.shape[2], lanes), 1) < rows_part
    for j in range(2):
        for h in range(side // per_line):
            u, w = sg[2 * h, j], sg[2 * h + 1, j]
            at = pl.ds(h * lanes, lanes)
            stat[j, 0, :, at] = jnp.where(low, u, pltpu.roll(w, rows_part, 1))
            stat[j, 1, :, at] = jnp.where(low, pltpu.roll(u, rows_part, 1), w)
    spot = lax.broadcasted_iota(jnp.int32, (1, tile_rows), 1)
    qpos0 = (sub_start + ((spot // sub_rows) % 2) * sub_len + (spot // n_heads) % local_len
             + ((y * side + spot // rows_part) * 2 + c) * local_len)

    def key_tile(t, _):
        yy, tt = lax.div(t, n_tiles), lax.rem(t, n_tiles)
        k0 = (yy * side + x) * pair + tt * kt
        line0 = lax.div(k0, lanes)
        keys = pl.ds(pl.multiple_of(tt * kt, kt), kt)
        lo = lax.div(jnp.maximum(k0 - sub_start, 0), span)
        last = jnp.max(ends[pl.ds(line0 + kt // lanes - 1, 1), :])
        hi = lax.div(jnp.maximum(last - sub_start + span, 0), span)

        @pl.when(hi > lo)
        def _():
            for g in range(kt // lanes):
                line = ends[pl.ds(line0 + g, 1), :]
                kcol[pl.ds(g * lanes, lanes), :] = jnp.broadcast_to(line, (lanes, lanes)).T

            def operands(i):
                part = pl.ds(pl.multiple_of(i * rows_part, rows_part), rows_part)
                q = jnp.concatenate([qg[s, 0, part, :] for s in range(side)], axis=0)
                do = jnp.concatenate([qg[s, 1, part, :] for s in range(side)], axis=0)
                return part, q, do

            def weigh(i, b):
                part, q, do = operands(i)
                g, odd = lax.div(i, 2), lax.rem(i, 2)
                k, v = kg[yy, 0, keys, :], kg[yy, 1, keys, :]
                lse, delta = stat[0, odd, pl.ds(g, 1), :], stat[1, odd, pl.ds(g, 1), :]
                qpos = qpos0 + i * span
                kend = jnp.concatenate([kcol[...]] * (tile_rows // lanes), axis=1)
                kpos = k0 + lax.broadcasted_iota(jnp.int32, (kt, tile_rows), 0)
                s_t = lax.dot_general(k, q, NT, preferred_element_type=jnp.float32)
                dp_t = lax.dot_general(v, do, NT, preferred_element_type=jnp.float32)
                p = jnp.exp2(s_t * (scale * LOG2E) - lse)
                p = jnp.where((kpos <= qpos) & (qpos <= kend), p, 0.0)
                pbuf[b][...] = p.astype(jnp.bfloat16)
                sbuf[b][...] = (p * (dp_t - delta)).astype(jnp.bfloat16)

            def spread(i, b):
                part, q, do = operands(i)
                ds = sbuf[b][...]
                dkv[yy, 1, keys, :] += lax.dot_general(pbuf[b][...], do, NN, preferred_element_type=jnp.float32)
                dkv[yy, 0, keys, :] += lax.dot_general(ds, q, NN, preferred_element_type=jnp.float32)
                dq_t = lax.dot_general(ds, kg[yy, 0, keys, :], TN, preferred_element_type=jnp.float32)
                for s in range(side):
                    dq[s, part, :] += dq_t[s * rows_part:(s + 1) * rows_part, :]

            weigh(lo, 0)

            def two_tiles(m, _):
                i = lo + 1 + 2 * m
                weigh(i, 1)
                spread(i - 1, 0)
                weigh(i + 1, 0)
                spread(i, 1)
                return 0

            n_twos = lax.div(hi - lo - 1, 2)
            lax.fori_loop(0, n_twos, two_tiles, 0)
            even = hi - lo - 1 > 2 * n_twos

            @pl.when(even)
            def _():
                weigh(hi - 1, 1)
                spread(hi - 2, 0)
                spread(hi - 1, 1)

            @pl.when(jnp.logical_not(even))
            def _():
                spread(hi - 1, 0)
        return 0

    lax.fori_loop(first_y * n_tiles, side * n_tiles, key_tile, 0)


def emit_kernel(a, b, c, out_a, out_b, out_c, sem):
    copies = [pltpu.make_async_copy(u, w, sem.at[i]) for i, (u, w) in enumerate(((a, out_a), (b, out_b), (c, out_c)))]
    for d in copies:
        d.start()
    for d in copies:
        d.wait()


def solution(mesh):
    cp_size = mesh.shape['cp']
    side = math.isqrt(cp_size // 2)
    assert side == 4 and side * side * 2 == cp_size
    q_spec = P(None, 'cp', 'tp', None)
    lse_spec = P(None, 'cp', 'tp')
    kv_spec = P('cp', 'tp', None)
    vspec = pl.BlockSpec(memory_space=VMEM)
    dma = pltpu.SemaphoreType.DMA

    def local_backward(query, out_act, out_grad, row_lse, key_act, value_act, doc_ids):
        n_sub, local_len, n_heads, head_dim = query.shape
        keys_local, n_kv = key_act.shape[0], key_act.shape[1]
        assert n_kv == 1
        f32, bf16 = jnp.float32, jnp.bfloat16
        sub_len = local_len * cp_size
        n_keys = keys_local * cp_size
        sub_start = n_keys - n_sub * sub_len
        scale = head_dim ** -0.5
        sub_rows = local_len * n_heads
        rows = n_sub * sub_rows
        pair = 2 * keys_local
        kt = 768
        lanes = 128
        st_shape = (2, rows // lanes, lanes)
        half = rows // 2
        n_part = 8
        kv_shape = (2, keys_local, head_dim)
        q_scratch = [VMEM((2, half, head_dim), f32), VMEM((2, rows, head_dim), f32), VMEM((2, half, head_dim), f32), dma((2, 6))]

        def run(first_y, ident, *arrays):
            qg, sg, kg, ends = pl.pallas_call(
                functools.partial(gather_kernel, side),
                out_shape=[jax.ShapeDtypeStruct((side, 2, rows, head_dim), bf16),
                           jax.ShapeDtypeStruct((side,) + st_shape, f32),
                           jax.ShapeDtypeStruct((side, 2, 2, keys_local, head_dim), bf16),
                           jax.ShapeDtypeStruct(arrays[-1].shape, jnp.int32)],
                in_specs=[vspec] * 7, out_specs=[vspec] * 4,
                scratch_shapes=[VMEM(st_shape, f32), VMEM((lanes, lanes), f32), dma((2, 6)), dma((2, 6)), dma((2, 5)), dma((2, 3)), dma((5,))],
                compiler_params=pltpu.CompilerParams(collective_id=ident, has_side_effects=True, vmem_limit_bytes=24 << 20),
                name='gather')(*arrays)

            tile_rows = side * 2 * sub_rows
            dq, dkv = pl.pallas_call(
                functools.partial(core_kernel, side, kt, sub_len, local_len, n_heads, sub_start, scale, first_y),
                out_shape=[jax.ShapeDtypeStruct((side, rows, head_dim), f32),
                           jax.ShapeDtypeStruct((side, 2, pair, head_dim), f32)],
                in_specs=[vspec] * 4, out_specs=[vspec] * 2,
                scratch_shapes=[VMEM((kt, lanes), jnp.int32), *[VMEM((kt, tile_rows), bf16)] * 4,
                                VMEM((2, 2, rows // lanes, tile_rows), f32)],
                compiler_params=pltpu.CompilerParams(vmem_limit_bytes=30 << 20),
                name='pairs')(ends, qg, sg, kg.reshape(side, 2, pair, head_dim))

            if first_y:
                body = functools.partial(reduce_upper_kernel, side, scale, 128, n_part)
                scratch = [VMEM((2,) + kv_shape, f32), VMEM((2,) + kv_shape, f32), *[VMEM(kv_shape, f32)] * 3,
                           *q_scratch, dma((2, 2 * n_part)), dma((2, n_part)), dma((2, n_part))]
            else:
                body = functools.partial(reduce_kernel, side, scale, 128)
                scratch = [VMEM((side,) + kv_shape, f32), VMEM((side,) + kv_shape, f32), VMEM(kv_shape, f32),
                           VMEM((2,) + kv_shape, f32), VMEM(kv_shape, f32), *q_scratch, dma((2, 6)), dma((2, 4))]
            return pl.pallas_call(
                body,
                out_shape=[jax.ShapeDtypeStruct((rows, head_dim), bf16),
                           jax.ShapeDtypeStruct((keys_local, head_dim), f32),
                           jax.ShapeDtypeStruct((keys_local, head_dim), f32)],
                in_specs=[vspec] * 2, out_specs=[vspec] * 3, scratch_shapes=scratch,
                compiler_params=pltpu.CompilerParams(collective_id=ident + 1, has_side_effects=True, vmem_limit_bytes=30 << 20),
                name='reduce')(dq, dkv.reshape(side, 2, 2, keys_local, head_dim))

        upper = side // 2
        recent = doc_ids[sub_start] - doc_ids[upper * side * pair - 1]
        flat = [t.reshape(rows, head_dim) for t in (query, out_grad, out_act)]
        lse = row_lse.transpose(1, 2, 0).reshape(sub_rows, n_sub)
        keys = [t.reshape(keys_local, head_dim) for t in (key_act, value_act)]
        sums = lax.switch(recent, [functools.partial(run, 0, 2), functools.partial(run, upper, 0)],
                          *flat, lse, *keys, doc_ids.reshape(n_keys // lanes, lanes))
        dq_out, dk, dv = pl.pallas_call(
            emit_kernel,
            out_shape=[jax.ShapeDtypeStruct(t.shape, t.dtype) for t in sums],
            in_specs=[vspec] * 3, out_specs=[pl.BlockSpec(memory_space=pl.ANY)] * 3,
            scratch_shapes=[dma((3,))],
            compiler_params=pltpu.CompilerParams(vmem_limit_bytes=16 << 20),
            name='emit')(*sums)
        return dq_out.reshape(query.shape), dk.reshape(key_act.shape), dv.reshape(value_act.shape)

    return jax.shard_map(local_backward, mesh=mesh, in_specs=(q_spec, q_spec, q_spec, lse_spec, kv_spec, kv_spec, P()), out_specs=(q_spec, kv_spec, kv_spec), check_vma=False)
```

```python
import functools
import math

import jax
import jax.numpy as jnp
from jax import lax
from jax.experimental import pallas as pl
from jax.experimental.pallas import tpu as pltpu
from jax.sharding import PartitionSpec as P

LOG2E = 1.4426950408889634
VMEM = pltpu.VMEM
NT = (((1,), (1,)), ((), ()))
NN = (((1,), (0,)), ((), ()))
TN = (((0,), (0,)), ((), ()))


def place(side):
    me = lax.axis_index('cp')
    return me // (2 * side), (me // 2) % side, me % 2


def rank_of(side, y, x, c):
    return {'cp': ((y % side) * side + (x % side)) * 2 + c}


def remote(src, dst, sems, i, to):
    return pltpu.make_async_remote_copy(
        src_ref=src, dst_ref=dst, send_sem=sems.at[0, i], recv_sem=sems.at[1, i],
        device_id=to, device_id_type=pl.DeviceIdType.MESH)


def greet(peers):
    barrier = pltpu.get_barrier_semaphore()
    for p in peers:
        pl.semaphore_signal(barrier, inc=1, device_id=p, device_id_type=pl.DeviceIdType.MESH)
    pl.semaphore_wait(barrier, len(peers))


def doc_ends(doc):
    n_rows, lanes = doc.shape
    far = n_rows * lanes
    row = lax.broadcasted_iota(jnp.int32, doc.shape, 0)
    lane = lax.broadcasted_iota(jnp.int32, doc.shape, 1)
    pos = row * lanes + lane
    below = pltpu.roll(doc, n_rows - 1, 0)
    after = jnp.where(lane == lanes - 1, pltpu.roll(below, lanes - 1, 1), pltpu.roll(doc, lanes - 1, 1))
    end = jnp.where((doc != after) | (pos == far - 1), pos, far)
    s = 1
    while s < lanes:
        end = jnp.minimum(end, jnp.where(lane < lanes - s, pltpu.roll(end, lanes - s, 1), far))
        s *= 2
    first = jnp.broadcast_to(end[:, 0:1], doc.shape)
    later = jnp.where(row < n_rows - 1, pltpu.roll(first, n_rows - 1, 0), far)
    s = 1
    while s < n_rows:
        later = jnp.minimum(later, jnp.where(row < n_rows - s, pltpu.roll(later, n_rows - s, 0), far))
        s *= 2
    return jnp.minimum(end, later)


def gather_kernel(side, early, late, q, do, out_hbm, lse_hbm, k, v, doc_hbm, qg, sg, kg, ends, gap, st, flip, out, lse, doc, sx, sy, sp, ss, sl):
    y, x, c = place(side)
    right, left = rank_of(side, y, x + 1, c), rank_of(side, y, x + side - 1, c)
    far = rank_of(side, y, x + 2, c)
    up, down = rank_of(side, y + 1, x, c), rank_of(side, y + side - 1, x, c)
    mate = rank_of(side, y, x, 1 - c)
    xl, xr, xf = (x + side - 1) % side, (x + 1) % side, (x + 2) % side
    yl, yr, yf = (y + side - 1) % side, (y + 1) % side, (y + 2) % side
    greet((right, left, far, up, down, mate))

    ya = remote(k, kg.at[y, 0, c], sy, 0, up)
    yc = remote(v, kg.at[y, 1, c], sy, 2, down)
    xa = remote(q, qg.at[x, 0], sx, 0, right)
    xc = remote(do, qg.at[x, 1], sx, 2, left)
    yb = remote(v, kg.at[y, 1, c], sy, 1, up)
    yd = remote(k, kg.at[y, 0, c], sy, 3, down)
    xb = remote(do, qg.at[x, 1], sx, 1, right)
    xd = remote(q, qg.at[x, 0], sx, 3, left)
    s0 = remote(st, sg.at[x], ss, 0, right)
    s1 = remote(st, sg.at[x], ss, 1, left)
    s2 = remote(st, sg.at[x], ss, 2, far)
    p0 = remote(k, kg.at[y, 0, c], sp, 0, mate)
    p4 = remote(v, kg.at[y, 1, c], sp, 4, mate)
    sends = [ya, yc, xa, xc, yb, yd, xb, xd, p0, p4]
    for d in sends:
        d.start()
    own = [pltpu.make_async_copy(q, qg.at[x, 0], sl.at[0]), pltpu.make_async_copy(do, qg.at[x, 1], sl.at[1]),
           pltpu.make_async_copy(k, kg.at[y, 0, c], sl.at[2]), pltpu.make_async_copy(v, kg.at[y, 1, c], sl.at[3]),
           pltpu.make_async_copy(st, sg.at[x], sl.at[4])]
    own += [pltpu.make_async_copy(u, w, sl.at[5 + i]) for i, (u, w) in enumerate(((out_hbm, out), (lse_hbm, lse), (doc_hbm, doc)))]
    for d in own[:4] + own[5:]:
        d.start()
    for d in own[5:] + own[1:2]:
        d.wait()
    lanes = st.shape[-1]
    sub_rows, n_sub = lse.shape
    flip[...] = jnp.zeros_like(flip)
    flip[pl.ds(0, sub_rows), pl.ds(0, n_sub)] = lse[...] * LOG2E
    flip[...] = flip[...].T
    folds = lanes // sub_rows
    lane = lax.broadcasted_iota(jnp.int32, (st.shape[1], lanes), 1)
    row_lse = jnp.zeros((st.shape[1], lanes), jnp.float32)
    for a in range(folds):
        some = flip[pl.ds(a, st.shape[1], stride=folds), :]
        some = pltpu.roll(some, a * sub_rows, 1) if a else some
        row_lse = jnp.where(lane // sub_rows == a, some, row_lse)
    st[0] = row_lse
    for g in range(st.shape[1]):
        rows = pl.ds(g * lanes, lanes)
        prod = qg[x, 1, rows, :].astype(jnp.float32) * out[rows, :].astype(jnp.float32)
        st[1, pl.ds(g, 1), :] = jnp.sum(prod.T, axis=0, keepdims=True)
    ends[...] = doc_ends(doc[...])
    step = doc[late // lanes, late % lanes] - doc[early // lanes, early % lanes]
    gap[0, 0] = jnp.minimum(step, 1)

    ya.wait_recv()
    ye = remote(kg.at[yl, 0, c], kg.at[yl, 0, c], sy, 4, up)
    ye.start()
    yc.wait_recv()
    yg = remote(kg.at[yr, 1, c], kg.at[yr, 1, c], sy, 5, down)
    yg.start()
    own[4].start()
    for d in (s0, s1, s2):
        d.start()
    xa.wait_recv()
    xe = remote(qg.at[xl, 0], qg.at[xl, 0], sx, 4, right)
    xe.start()
    xc.wait_recv()
    xg = remote(qg.at[xr, 1], qg.at[xr, 1], sx, 5, left)
    xg.start()
    yb.wait_recv()
    p1 = remote(kg.at[yl, :, c], kg.at[yl, :, c], sp, 1, mate)
    p1.start()
    yd.wait_recv()
    p2 = remote(kg.at[yr, :, c], kg.at[yr, :, c], sp, 2, mate)
    p2.start()
    ye.wait_recv()
    yg.wait_recv()
    p3 = remote(kg.at[yf, :, c], kg.at[yf, :, c], sp, 3, mate)
    p3.start()
    for d in (xb, xd, xe, xg, s0, s1, s2, p0, p1, p2, p3, p4):
        d.wait_recv()
    for d in (own[0], own[2], own[3], own[4]):
        d.wait()
    for d in sends + [s0, s1, s2, ye, yg, xe, xg, p1, p2, p3]:
        d.wait_send()


def reduce_kernel(side, scale, chunk, dq, dkv, dq_out, dk_out, dv_out,
                  pc, acc, ka, kb, kt, qa, qb, qt, sx, sy, sp):
    y, x, c = place(side)
    right, left = rank_of(side, y, x + 1, c), rank_of(side, y, x + side - 1, c)
    up, down = rank_of(side, y + 1, x, c), rank_of(side, y + side - 1, x, c)
    mate = rank_of(side, y, x, 1 - c)
    xl, xr, xf = (x + side - 1) % side, (x + 1) % side, (x + 2) % side
    yl, yr, yf = (y + side - 1) % side, (y + 1) % side, (y + 2) % side
    half = dq.shape[1] // 2
    h0, h1 = pl.ds(0, half), pl.ds(half, half)
    greet((right, left, up, down, mate))

    def add(out, a, b):
        def step(i, _):
            rows = pl.ds(pl.multiple_of(i * chunk, chunk), chunk)
            out[rows, :] = a[rows, :] + b[rows, :]
            return 0
        lax.fori_loop(0, out.shape[0] // chunk, step, 0)

    slots = (yf, yr, yl, y)
    mates = [remote(dkv.at[s, :, 1 - c], pc.at[s], sp, i, mate) for i, s in enumerate(slots)]
    xa = remote(dq.at[xf, h0], qa.at[0], sx, 0, right)
    xc = remote(dq.at[xf, h1], qa.at[1], sx, 1, left)
    xb = remote(dq.at[xr, h1], qb.at[0, h1], sx, 2, right)
    xd = remote(dq.at[xl, h0], qb.at[1, h0], sx, 3, left)
    sends = [mates[0], xa, xc, mates[1], mates[2], mates[3], xb, xd]
    for d in sends:
        d.start()

    mates[0].wait_recv()
    for j in range(2):
        add(acc.at[yf, j], dkv.at[yf, j, c], pc.at[yf, j])
    ya = remote(acc.at[yf, 0], ka.at[0], sy, 0, up)
    yc = remote(acc.at[yf, 1], ka.at[1], sy, 1, down)
    ya.start()
    yc.start()
    mates[1].wait_recv()
    mates[2].wait_recv()
    add(acc.at[yr, 1], dkv.at[yr, 1, c], pc.at[yr, 1])
    yb = remote(acc.at[yr, 1], kb.at[0, 1], sy, 2, up)
    yb.start()
    add(acc.at[yl, 0], dkv.at[yl, 0, c], pc.at[yl, 0])
    yd = remote(acc.at[yl, 0], kb.at[1, 0], sy, 3, down)
    yd.start()
    add(acc.at[yr, 0], dkv.at[yr, 0, c], pc.at[yr, 0])
    add(acc.at[yl, 1], dkv.at[yl, 1, c], pc.at[yl, 1])
    mates[3].wait_recv()
    for j in range(2):
        add(acc.at[y, j], dkv.at[y, j, c], pc.at[y, j])

    xa.wait_recv()
    add(qt.at[0], dq.at[xr, h0], qa.at[0])
    xe = remote(qt.at[0], qb.at[0, h0], sx, 4, right)
    xe.start()
    xc.wait_recv()
    add(qt.at[1], dq.at[xl, h1], qa.at[1])
    xg = remote(qt.at[1], qb.at[1, h1], sx, 5, left)
    xg.start()
    ya.wait_recv()
    add(kt.at[0], acc.at[yr, 0], ka.at[0])
    ye = remote(kt.at[0], kb.at[0, 0], sy, 4, up)
    ye.start()
    yc.wait_recv()
    add(kt.at[1], acc.at[yl, 1], ka.at[1])
    yg = remote(kt.at[1], kb.at[1, 1], sy, 5, down)
    yg.start()

    for d in (xb, xd, xe, xg):
        d.wait_recv()

    def fin_q(i, _):
        rows = pl.ds(pl.multiple_of(i * chunk, chunk), chunk)
        total = dq[x, rows, :] + qb[0, rows, :] + qb[1, rows, :]
        dq_out[rows, :] = (total * scale).astype(dq_out.dtype)
        return 0

    lax.fori_loop(0, dq_out.shape[0] // chunk, fin_q, 0)
    for d in (yb, yd, ye, yg):
        d.wait_recv()

    def fin_k(i, _):
        rows = pl.ds(pl.multiple_of(i * chunk, chunk), chunk)
        dk_out[rows, :] = (acc[y, 0, rows, :] + kb[0, 0, rows, :] + kb[1, 0, rows, :]) * scale
        dv_out[rows, :] = acc[y, 1, rows, :] + kb[0, 1, rows, :] + kb[1, 1, rows, :]
        return 0

    lax.fori_loop(0, dk_out.shape[0] // chunk, fin_k, 0)
    for d in sends + [ya, yc, yb, yd, ye, yg, xe, xg]:
        d.wait_send()


def reduce_upper_kernel(side, scale, chunk, n_part, dq, dkv, dq_out, dk_out, dv_out,
                        pc, acc, got, tot, end, qa, qb, qt, sx, sp, s1, s2):
    y, x, c = place(side)
    right, left = rank_of(side, y, x + 1, c), rank_of(side, y, x + side - 1, c)
    up, down = rank_of(side, y + 1, x, c), rank_of(side, y + side - 1, x, c)
    mate = rank_of(side, y, x, 1 - c)
    beside = rank_of(side, y + 1 - 2 * (y % 2), x, c)
    across = rank_of(side, side - 1 - y, x, c)
    xl, xr, xf = (x + side - 1) % side, (x + 1) % side, (x + 2) % side
    give = side // 2 + (y + y // 2) % 2
    keep = side + 1 - give
    lower = y < side // 2
    half = dq.shape[1] // 2
    h0, h1 = pl.ds(0, half), pl.ds(half, half)
    per = dkv.shape[3] // (n_part // 2)
    parts = [(i % 2, pl.ds((i // 2) * per, per)) for i in range(n_part)]
    greet((right, left, up, down, mate))

    def add(out, a, b):
        def step(i, _):
            rows = pl.ds(pl.multiple_of(i * chunk, chunk), chunk)
            out[rows, :] = a[rows, :] + b[rows, :]
            return 0
        lax.fori_loop(0, out.shape[0] // chunk, step, 0)

    m1 = [remote(dkv.at[give, j, 1 - c, r], pc.at[0, j, r], sp, i, mate) for i, (j, r) in enumerate(parts)]
    m2 = [remote(dkv.at[keep, j, 1 - c, r], pc.at[1, j, r], sp, n_part + i, mate) for i, (j, r) in enumerate(parts)]
    xa = remote(dq.at[xf, h0], qa.at[0], sx, 0, right)
    xc = remote(dq.at[xf, h1], qa.at[1], sx, 1, left)
    xb = remote(dq.at[xr, h1], qb.at[0, h1], sx, 2, right)
    xd = remote(dq.at[xl, h0], qb.at[1, h0], sx, 3, left)
    sends = m1 + [xa, xc] + m2 + [xb, xd]
    for d in sends:
        d.start()

    k1 = [remote(acc.at[0, j, r], got.at[j, r], s1, i, beside) for i, (j, r) in enumerate(parts)]
    k2 = [remote(tot.at[j, r], end.at[j, r], s2, i, across) for i, (j, r) in enumerate(parts)]
    for i, (j, r) in enumerate(parts):
        m1[i].wait_recv()
        acc[0, j, r, :] = dkv[give, j, c, r, :] + pc[0, j, r, :]
        k1[i].start()
    for i, (j, r) in enumerate(parts):
        m2[i].wait_recv()
        acc[1, j, r, :] = dkv[keep, j, c, r, :] + pc[1, j, r, :]
    for i, (j, r) in enumerate(parts):
        k1[i].wait_recv()
        tot[j, r, :] = acc[1, j, r, :] + got[j, r, :]

        @pl.when(lower)
        def _():
            k2[i].start()

        if i == 1:
            xa.wait_recv()
            add(qt.at[0], dq.at[xr, h0], qa.at[0])
            xe = remote(qt.at[0], qb.at[0, h0], sx, 4, right)
            xe.start()
            xc.wait_recv()
            add(qt.at[1], dq.at[xl, h1], qa.at[1])
            xg = remote(qt.at[1], qb.at[1, h1], sx, 5, left)
            xg.start()

    for d in (xb, xd, xe, xg):
        d.wait_recv()

    def fin_q(i, _):
        rows = pl.ds(pl.multiple_of(i * chunk, chunk), chunk)
        total = dq[x, rows, :] + qb[0, rows, :] + qb[1, rows, :]
        dq_out[rows, :] = (total * scale).astype(dq_out.dtype)
        return 0

    lax.fori_loop(0, dq_out.shape[0] // chunk, fin_q, 0)

    @pl.when(jnp.logical_not(lower))
    def _():
        for i, (j, r) in enumerate(parts):
            k2[i].wait_recv()
            if j == 0:
                dk_out[r, :] = (tot[j, r, :] + end[j, r, :]) * scale
            else:
                dv_out[r, :] = tot[j, r, :] + end[j, r, :]

    @pl.when(lower)
    def _():
        dk_out[...] = jnp.zeros_like(dk_out)
        dv_out[...] = jnp.zeros_like(dv_out)
        for d in k2:
            d.wait_send()

    for d in sends + k1 + [xe, xg]:
        d.wait_send()


def core_kernel(side, kt, sub_len, local_len, n_heads, sub_start, scale, first_y, ends, qg, sg, kg, dq, dkv, kcol, pbuf0, pbuf1, sbuf0, sbuf1, stat):
    pbuf, sbuf = (pbuf0, pbuf1), (sbuf0, sbuf1)
    y, x, c = place(side)
    pair = kg.shape[2]
    n_tiles = pair // kt
    sub_rows = local_len * n_heads
    rows_part = 2 * sub_rows
    tile_rows = side * rows_part
    span = 2 * sub_len
    lanes = 128
    dq[...] = jnp.zeros_like(dq)
    for yy in range(first_y, side):
        dkv[yy] = jnp.zeros(dkv.shape[1:], dkv.dtype)
    per_line = lanes // rows_part
    low = lax.broadcasted_iota(jnp.int32, (stat.shape[2], lanes), 1) < rows_part
    for j in range(2):
        for h in range(side // per_line):
            u, w = sg[2 * h, j], sg[2 * h + 1, j]
            at = pl.ds(h * lanes, lanes)
            stat[j, 0, :, at] = jnp.where(low, u, pltpu.roll(w, rows_part, 1))
            stat[j, 1, :, at] = jnp.where(low, pltpu.roll(u, rows_part, 1), w)
    spot = lax.broadcasted_iota(jnp.int32, (1, tile_rows), 1)
    qpos0 = (sub_start + ((spot // sub_rows) % 2) * sub_len + (spot // n_heads) % local_len
             + ((y * side + spot // rows_part) * 2 + c) * local_len)

    def key_tile(t, _):
        yy, tt = lax.div(t, n_tiles), lax.rem(t, n_tiles)
        k0 = (yy * side + x) * pair + tt * kt
        line0 = lax.div(k0, lanes)
        keys = pl.ds(pl.multiple_of(tt * kt, kt), kt)
        lo = lax.div(jnp.maximum(k0 - sub_start, 0), span)
        last = jnp.max(ends[pl.ds(line0 + kt // lanes - 1, 1), :])
        hi = lax.div(jnp.maximum(last - sub_start + span, 0), span)

        @pl.when(hi > lo)
        def _():
            for g in range(kt // lanes):
                line = ends[pl.ds(line0 + g, 1), :]
                kcol[pl.ds(g * lanes, lanes), :] = jnp.broadcast_to(line, (lanes, lanes)).T

            def operands(i):
                part = pl.ds(pl.multiple_of(i * rows_part, rows_part), rows_part)
                q = jnp.concatenate([qg[s, 0, part, :] for s in range(side)], axis=0)
                do = jnp.concatenate([qg[s, 1, part, :] for s in range(side)], axis=0)
                return part, q, do

            def weigh(i, b):
                part, q, do = operands(i)
                g, odd = lax.div(i, 2), lax.rem(i, 2)
                k, v = kg[yy, 0, keys, :], kg[yy, 1, keys, :]
                lse, delta = stat[0, odd, pl.ds(g, 1), :], stat[1, odd, pl.ds(g, 1), :]
                qpos = qpos0 + i * span
                kend = jnp.concatenate([kcol[...]] * (tile_rows // lanes), axis=1)
                kpos = k0 + lax.broadcasted_iota(jnp.int32, (kt, tile_rows), 0)
                s_t = lax.dot_general(k, q, NT, preferred_element_type=jnp.float32)
                dp_t = lax.dot_general(v, do, NT, preferred_element_type=jnp.float32)
                p = jnp.exp2(s_t * (scale * LOG2E) - lse)
                p = jnp.where((kpos <= qpos) & (qpos <= kend), p, 0.0)
                pbuf[b][...] = p.astype(jnp.bfloat16)
                sbuf[b][...] = (p * (dp_t - delta)).astype(jnp.bfloat16)

            def spread(i, b):
                part, q, do = operands(i)
                ds = sbuf[b][...]
                dkv[yy, 1, keys, :] += lax.dot_general(pbuf[b][...], do, NN, preferred_element_type=jnp.float32)
                dkv[yy, 0, keys, :] += lax.dot_general(ds, q, NN, preferred_element_type=jnp.float32)
                dq_t = lax.dot_general(ds, kg[yy, 0, keys, :], TN, preferred_element_type=jnp.float32)
                for s in range(side):
                    dq[s, part, :] += dq_t[s * rows_part:(s + 1) * rows_part, :]

            weigh(lo, 0)

            def two_tiles(m, _):
                i = lo + 1 + 2 * m
                weigh(i, 1)
                spread(i - 1, 0)
                weigh(i + 1, 0)
                spread(i, 1)
                return 0

            n_twos = lax.div(hi - lo - 1, 2)
            lax.fori_loop(0, n_twos, two_tiles, 0)
            even = hi - lo - 1 > 2 * n_twos

            @pl.when(even)
            def _():
                weigh(hi - 1, 1)
                spread(hi - 2, 0)
                spread(hi - 1, 1)

            @pl.when(jnp.logical_not(even))
            def _():
                spread(hi - 1, 0)
        return 0

    lax.fori_loop(first_y * n_tiles, side * n_tiles, key_tile, 0)


def emit_kernel(a, b, c, out_a, out_b, out_c, sem):
    copies = [pltpu.make_async_copy(u, w, sem.at[i]) for i, (u, w) in enumerate(((a, out_a), (b, out_b), (c, out_c)))]
    for d in copies:
        d.start()
    for d in copies:
        d.wait()


def solution(mesh):
    cp_size = mesh.shape['cp']
    side = math.isqrt(cp_size // 2)
    assert side == 4 and side * side * 2 == cp_size
    q_spec = P(None, 'cp', 'tp', None)
    lse_spec = P(None, 'cp', 'tp')
    kv_spec = P('cp', 'tp', None)
    vspec = pl.BlockSpec(memory_space=VMEM)
    dma = pltpu.SemaphoreType.DMA

    def local_backward(query, out_act, out_grad, row_lse, key_act, value_act, doc_ids):
        n_sub, local_len, n_heads, head_dim = query.shape
        keys_local, n_kv = key_act.shape[0], key_act.shape[1]
        assert n_kv == 1
        f32, bf16 = jnp.float32, jnp.bfloat16
        sub_len = local_len * cp_size
        n_keys = keys_local * cp_size
        sub_start = n_keys - n_sub * sub_len
        scale = head_dim ** -0.5
        sub_rows = local_len * n_heads
        rows = n_sub * sub_rows
        pair = 2 * keys_local
        kt = 768
        lanes = 128
        st_shape = (2, rows // lanes, lanes)
        half = rows // 2
        n_part = 8
        kv_shape = (2, keys_local, head_dim)
        q_scratch = [VMEM((2, half, head_dim), f32), VMEM((2, rows, head_dim), f32), VMEM((2, half, head_dim), f32), dma((2, 6))]

        def run(first_y, ident, ends, qg, sg, kg):
            tile_rows = side * 2 * sub_rows
            dq, dkv = pl.pallas_call(
                functools.partial(core_kernel, side, kt, sub_len, local_len, n_heads, sub_start, scale, first_y),
                out_shape=[jax.ShapeDtypeStruct((side, rows, head_dim), f32),
                           jax.ShapeDtypeStruct((side, 2, pair, head_dim), f32)],
                in_specs=[vspec] * 4, out_specs=[vspec] * 2,
                scratch_shapes=[VMEM((kt, lanes), jnp.int32), *[VMEM((kt, tile_rows), bf16)] * 4,
                                VMEM((2, 2, rows // lanes, tile_rows), f32)],
                compiler_params=pltpu.CompilerParams(vmem_limit_bytes=30 << 20),
                name='pairs')(ends, qg, sg, kg.reshape(side, 2, pair, head_dim))

            if first_y:
                body = functools.partial(reduce_upper_kernel, side, scale, 128, n_part)
                scratch = [VMEM((2,) + kv_shape, f32), VMEM((2,) + kv_shape, f32), *[VMEM(kv_shape, f32)] * 3,
                           *q_scratch, dma((2, 2 * n_part)), dma((2, n_part)), dma((2, n_part))]
            else:
                body = functools.partial(reduce_kernel, side, scale, 128)
                scratch = [VMEM((side,) + kv_shape, f32), VMEM((side,) + kv_shape, f32), VMEM(kv_shape, f32),
                           VMEM((2,) + kv_shape, f32), VMEM(kv_shape, f32), *q_scratch, dma((2, 6)), dma((2, 4))]
            return pl.pallas_call(
                body,
                out_shape=[jax.ShapeDtypeStruct((rows, head_dim), bf16),
                           jax.ShapeDtypeStruct((keys_local, head_dim), f32),
                           jax.ShapeDtypeStruct((keys_local, head_dim), f32)],
                in_specs=[vspec] * 2, out_specs=[vspec] * 3, scratch_shapes=scratch,
                compiler_params=pltpu.CompilerParams(collective_id=ident, has_side_effects=True, vmem_limit_bytes=30 << 20),
                name='reduce')(dq, dkv.reshape(side, 2, 2, keys_local, head_dim))

        upper = side // 2
        flat = [t.reshape(rows, head_dim) for t in (query, out_grad, out_act)]
        lse = row_lse.transpose(1, 2, 0).reshape(sub_rows, n_sub)
        keys = [t.reshape(keys_local, head_dim) for t in (key_act, value_act)]
        qg, sg, kg, ends, gap = pl.pallas_call(
            functools.partial(gather_kernel, side, upper * side * pair - 1, sub_start),
            out_shape=[jax.ShapeDtypeStruct((side, 2, rows, head_dim), bf16),
                       jax.ShapeDtypeStruct((side,) + st_shape, f32),
                       jax.ShapeDtypeStruct((side, 2, 2, keys_local, head_dim), bf16),
                       jax.ShapeDtypeStruct((n_keys // lanes, lanes), jnp.int32),
                       jax.ShapeDtypeStruct((1, 1), jnp.int32)],
            in_specs=[pl.BlockSpec(memory_space=pltpu.HBM)] * 7, out_specs=[vspec] * 4 + [pl.BlockSpec(memory_space=pltpu.SMEM)],
            scratch_shapes=[VMEM(st_shape, f32), VMEM((lanes, lanes), f32), VMEM((rows, head_dim), bf16), VMEM(lse.shape, f32), VMEM((n_keys // lanes, lanes), jnp.int32), dma((2, 6)), dma((2, 6)), dma((2, 5)), dma((2, 3)), dma((8,))],
            compiler_params=pltpu.CompilerParams(collective_id=0, has_side_effects=True, vmem_limit_bytes=61120000),
            name='gather')(*flat, lse, *keys, doc_ids.reshape(n_keys // lanes, lanes))

        sums = lax.switch(gap[0, 0], [functools.partial(run, 0, 1), functools.partial(run, upper, 2)], ends, qg, sg, kg)
        dq_out, dk, dv = pl.pallas_call(
            emit_kernel,
            out_shape=[jax.ShapeDtypeStruct(t.shape, t.dtype) for t in sums],
            in_specs=[vspec] * 3, out_specs=[pl.BlockSpec(memory_space=pl.ANY)] * 3,
            scratch_shapes=[dma((3,))],
            compiler_params=pltpu.CompilerParams(vmem_limit_bytes=16 << 20),
            name='emit')(*sums)
        return dq_out.reshape(query.shape), dk.reshape(key_act.shape), dv.reshape(value_act.shape)

    return jax.shard_map(local_backward, mesh=mesh, in_specs=(q_spec, q_spec, q_spec, lse_spec, kv_spec, kv_spec, P()), out_specs=(q_spec, kv_spec, kv_spec), check_vma=False)
```
